32 devices in a mesh: band: 8 (over z, y), grid: 4 (over x, core).
Axes of the slice: x: 2, y: 2, z: 4, core: 2. Of those that a mesh axis runs over, the one named last changes fastest.
Arguments:
- orbitals: float32 [24, 64, 4096], P('band', 'grid'), may hold values from -6 to 6
- pair_mask: int32 [24, 24], replicated, may hold values from 0 to 1, as said below
Outputs:
- exchange_term: float32 [24, 64, 4096], P('band', 'grid')
The draws below stay inside these ranges and needn't reach their ends.
Inputs may be any that keep to these rules, and one draw needn't show every extreme that they name: pair_mask is symmetric; entries outside the candidate pairs of every block (and their transposes) are 0; each block has at most 12 candidate pairs with mask 1, and some block has exactly 12.
All inputs are finite; a program needn't handle non-finite values.
Results may differ from the reference program's by a relative error of at most 0.00027.
Values sent between devices are 32-bit elements; how exact they have to be, the bound alone decides.
A program may use at most 64 MiB of HBM per device.

```python
import math
import jax
import jax.numpy as jnp
import numpy as np
from jax import lax

NG = 64
ORB_DEV = 3
REACH = 2
NORB = 24
NCAND = 24
CAP = 12


def pair_table_drawn():
    entries = []
    for distance in range(REACH + 1):
        for leading_orbital in range(ORB_DEV):
            for second_orb in range(ORB_DEV):
                if distance > 0 or leading_orbital <= second_orb:
                    entries.append((leading_orbital, distance, second_orb))
    return np.array(entries, dtype=np.int32)


def draw_orbitals(key, part):
    full_shape = (NORB, NG, NG * NG)
    values_out = jax.random.normal(key, full_shape, jnp.float32)
    return jnp.clip(values_out, -6.0, 6.0)


def draw_pair_mask(key, part):
    pair_list = pair_table_drawn()
    groups = NORB // ORB_DEV
    key_counts, key_full, key_scores = jax.random.split(jax.random.fold_in(key, 17), 3)
    counts = jax.random.randint(key_counts, (groups,), 1, CAP + 1)
    full_group = jax.random.randint(key_full, (), 0, groups)
    counts = jnp.where(jnp.arange(groups, dtype=jnp.int32) == full_group, CAP, counts)
    scores = jax.random.randint(key_scores, (groups, NCAND), 0, 1 << 20) * NCAND + jnp.arange(NCAND, dtype=jnp.int32)[None, :]
    ranks = jnp.argsort(jnp.argsort(scores, axis=1), axis=1)
    live_flags = (ranks < counts[:, None]).astype(jnp.int32)
    group_ids = jnp.arange(groups, dtype=jnp.int32)[:, None]
    row_ids = group_ids * ORB_DEV + jnp.asarray(pair_list[:, 0])[None, :]
    col_ids = (group_ids + jnp.asarray(pair_list[:, 1])[None, :]) % groups * ORB_DEV + jnp.asarray(pair_list[:, 2])[None, :]
    mask_out = jnp.zeros((NORB, NORB), jnp.int32)
    mask_out = mask_out.at[row_ids.reshape(-1), col_ids.reshape(-1)].set(live_flags.reshape(-1))
    mask_out = mask_out.at[col_ids.reshape(-1), row_ids.reshape(-1)].set(live_flags.reshape(-1))
    return mask_out


def setup_inputs(seed: int = 0) -> dict:
    key_list = jax.random.split(jax.random.key(seed), 3)
    return {
        "orbitals": draw_orbitals(jax.random.fold_in(key_list[2], 71), 0),
        "pair_mask": draw_pair_mask(jax.random.fold_in(key_list[2], 71), 0),
    }


MIXING = 0.25
BOX_LENGTH = 16.0


def pair_table():
    entries = []
    for distance in range(REACH + 1):
        for leading_orbital in range(ORB_DEV):
            for second_orb in range(ORB_DEV):
                if distance > 0 or leading_orbital <= second_orb:
                    entries.append((leading_orbital, distance, second_orb))
    return np.array(entries, dtype=np.int32)


def poisson_green_kernel():
    positions = jnp.arange(NG, dtype=jnp.int32)
    signed_waves = jnp.where(positions < NG // 2, positions, positions - NG)
    squared = (signed_waves[:, None, None] ** 2 + signed_waves[None, :, None] ** 2
               + signed_waves[None, None, :] ** 2)
    safe_values = jnp.maximum(squared, 1).astype(jnp.float32)
    return jnp.where(squared > 0, jnp.float32(BOX_LENGTH * BOX_LENGTH / math.pi) / safe_values,
                     jnp.float32(0.0))


def reference(orbitals, pair_mask):
    groups = NORB // ORB_DEV
    pair_list = pair_table()
    band_ids = np.arange(groups, dtype=np.int32)[:, None]
    row_ids = (band_ids * ORB_DEV + pair_list[None, :, 0]).reshape(-1).astype(np.int32)
    col_ids = (((band_ids + pair_list[None, :, 1]) % groups) * ORB_DEV
               + pair_list[None, :, 2]).reshape(-1).astype(np.int32)
    weights = pair_mask[jnp.asarray(row_ids), jnp.asarray(col_ids)].astype(jnp.float32)
    cross_flags = jnp.asarray((row_ids != col_ids).astype(np.float32)).astype(jnp.float32)
    cubes = orbitals.reshape(NORB, NG, NG, NG)
    kernel = poisson_green_kernel()

    def one_pair(totals, pair_input):
        row_id, col_id, weight, cross_flag = pair_input
        first_cube = cubes[row_id]
        second_cube = cubes[col_id]
        potential = jnp.real(jnp.fft.ifftn(jnp.fft.fftn(first_cube * second_cube) * kernel))
        totals = totals.at[row_id].add(weight * potential * second_cube)
        totals = totals.at[col_id].add(weight * cross_flag * potential * first_cube)
        return totals, None

    totals, discarded_value = lax.scan(one_pair, jnp.zeros((NORB, NG, NG, NG), jnp.float32),
                              (jnp.asarray(row_ids).astype(jnp.int32), jnp.asarray(col_ids).astype(jnp.int32),
                               weights, cross_flags))
    return (-MIXING * totals).reshape(NORB, NG, NG * NG)
```

```python
import functools
import math

import jax
import jax.numpy as jnp
import numpy as np
from jax import lax
from jax.experimental import pallas as pl
from jax.experimental.pallas import tpu as pltpu
from jax.sharding import PartitionSpec as P

MESH = pl.DeviceIdType.MESH
MIXING = 0.25
BOX_LENGTH = 16.0
UNROLL = 16
SKEW = 4

PEER, CROSS, RELAY, DOWN, SIDE, SIDE_BACK, UP_BACK, REDUCE = 0, 3, 6, 9, 13, 17, 21, 25
COPIES = 34


def transform_tables(n):
    ids = np.arange(n)
    angles = (ids[:, None] * ids[None, :] % n) * (2.0 * np.pi / n)
    cas = np.cos(angles) + np.sin(angles)
    high = cas.astype(jnp.bfloat16).astype(np.float64)
    low = cas - high
    none = np.zeros_like(high)
    left = np.block([[high, high], [low, none]])
    both = lambda m: np.block([[m, none], [none, m]])
    right = np.block([[both(high), both(low)], [both(high), np.zeros((2 * n, 2 * n))]])
    return jnp.asarray(left, jnp.bfloat16), jnp.asarray(right, jnp.bfloat16)


def split(values, axis):
    high = values.astype(jnp.bfloat16)
    low = (values - high.astype(jnp.float32)).astype(jnp.bfloat16)
    return jnp.concatenate([high, low], axis=axis)


def left_product(left, values):
    both = jnp.dot(left, split(values, 0), preferred_element_type=jnp.float32)
    half = both.shape[0] // 2
    return both[:half] + both[half:]


def right_product(values, right):
    both = jnp.dot(split(values, 1), right, preferred_element_type=jnp.float32)
    half = both.shape[1] // 2
    return both[:, :half] + both[:, half:]


def fill_coulomb(n, coulomb):
    lanes = 2 * n
    scale = -MIXING * BOX_LENGTH * BOX_LENGTH / math.pi / float(n**3)

    def signed(index):
        return jnp.where(index < n // 2, index, index - n)

    def body(kx, carry):
        fx = signed(kx)
        fy = signed(lax.broadcasted_iota(jnp.int32, (n, lanes), 0))
        fz = signed(lax.broadcasted_iota(jnp.int32, (n, lanes), 1) % n)
        squared = fx * fx + fy * fy + fz * fz
        safe = jnp.maximum(squared, 1).astype(jnp.float32)
        coulomb[pl.ds(pl.multiple_of(kx * n, n), n), :] = jnp.where(squared > 0, scale / safe, 0.0)
        return carry

    lax.fori_loop(0, n, body, 0)


def potentials(n, phi, pot, coulomb, work, left_ref, right_ref, pairs):
    lanes, half, stride = 2 * n, n // 2, n + SKEW
    unroll = min(UNROLL, half)
    (ia, ta, wa, ca), (ib, tb, wb, cb) = pairs
    lower = lax.broadcasted_iota(jnp.int32, (n, lanes), 1) < n

    def cols(c):
        return pl.ds(pl.multiple_of(c * lanes, lanes), lanes)

    def forward(step, carry):
        left, right = left_ref[...], right_ref[...]
        rows = []
        for u in range(unroll):
            c = step * unroll + u
            first = phi[ia, :, cols(c)] * phi[ta, :, cols(c)] * wa
            second = phi[ib, :, cols(c)] * phi[tb, :, cols(c)] * wb
            turned = pltpu.roll(jnp.where(lower, second, first), n, 1)
            rows += [jnp.where(lower, first, turned), jnp.where(lower, turned, second)]
        along_z = right_product(jnp.concatenate(rows, axis=0), right)
        for u in range(unroll):
            c = step * unroll + u
            even, odd = along_z[2 * u * n:(2 * u + 1) * n], along_z[(2 * u + 1) * n:(2 * u + 2) * n]
            along_x = left_product(left, jnp.concatenate([even, odd], axis=1))
            work[pl.ds(2 * c * stride, n), :] = along_x[:, :lanes]
            work[pl.ds((2 * c + 1) * stride, n), :] = along_x[:, lanes:]
        return carry

    def middle(step, carry):
        left = left_ref[...]
        for u in range(unroll):
            kx = (step * unroll + u) * 2
            here = [pl.ds(kx + j, n, stride=stride) for j in range(2)]
            factor = [coulomb[pl.ds(pl.multiple_of((kx + j) * n, n), n), :] for j in range(2)]
            spectrum = left_product(left, jnp.concatenate([work[h, :] for h in here], axis=1))
            solved = left_product(left, spectrum * jnp.concatenate(factor, axis=1))
            work[here[0], :] = solved[:, :lanes]
            work[here[1], :] = solved[:, lanes:]
        return carry

    def inverse(step, carry):
        left, right = left_ref[...], right_ref[...]
        rows = []
        for u in range(unroll):
            c = step * unroll + u
            planes = [work[pl.ds((2 * c + j) * stride, n), :] for j in range(2)]
            along_x = left_product(left, jnp.concatenate(planes, axis=1))
            rows += [along_x[:, :lanes], along_x[:, lanes:]]
        along_z = right_product(jnp.concatenate(rows, axis=0), right)
        for u in range(unroll):
            c = step * unroll + u
            even, odd = along_z[2 * u * n:(2 * u + 1) * n], along_z[(2 * u + 1) * n:(2 * u + 2) * n]
            turned = pltpu.roll(jnp.where(lower, odd, even), n, 1)
            found = (jnp.where(lower, even, turned), jnp.where(lower, turned, odd))
            for value, (i, t, _, cross) in zip(found, pairs):
                pot[i, :, cols(c)] += value * phi[t, :, cols(c)]
                pot[t, :, cols(c)] += value * phi[i, :, cols(c)] * cross
        return carry

    lax.fori_loop(0, half // unroll, forward, 0)
    lax.fori_loop(0, half // unroll, middle, 0)
    lax.fori_loop(0, half // unroll, inverse, 0)


def kernel(groups, mask_ref, mine_ref, left_ref, right_ref, out_ref,
           phi, pot, coulomb, work, side, up, red, send_sem, recv_sem):
    orbs, planes, cells = mine_ref.shape
    n = phi.shape[1]
    band, grid = lax.axis_index("band"), lax.axis_index("grid")
    last = grid // orbs
    odd_band = lax.rem(band, 2)
    below, above = lax.rem(band + groups - 2, groups), lax.rem(band + 2, groups)
    beside = band + 1 - 2 * odd_band
    peer, across, far = grid + 1 - 2 * lax.rem(grid, 2), lax.rem(grid + 2, 4), 3 - grid
    other = {1: peer, 2: across, 3: far}
    shares = grid < orbs
    even_shares = shares & (odd_band == 0)
    odd_shares = shares & (odd_band == 1)

    def order(device):
        first = device - device // orbs
        second = 1 - (device + 2) // orbs
        return first, second, orbs - first - second

    def rows(quarter):
        return pl.ds(pl.multiple_of(quarter * planes, planes), planes)

    def copy(source, target, number, device):
        return pltpu.make_async_remote_copy(
            src_ref=source, dst_ref=target, send_sem=send_sem.at[number], recv_sem=recv_sem.at[number],
            device_id=device, device_id_type=MESH)

    def arrived(target, number):
        copy(target, target, number, (band, peer)).wait_recv()

    def left_here(target, number):
        copy(target, target, number, (band, peer)).wait_send()

    barrier = pltpu.get_barrier_semaphore()
    for device in ((band, peer), (band, across), (band, far), (beside, grid), (below, grid), (above, grid)):
        pl.semaphore_signal(barrier, inc=1, device_id=device, device_id_type=MESH)
    pl.semaphore_wait(barrier, 6)

    quarters = (grid, peer, across, far)

    def pass_on(k, source):
        @pl.when(shares)
        def _():
            copy(source, phi.at[4, rows(quarters[k])], DOWN + k, (below, grid)).start()

        @pl.when(odd_shares)
        def _():
            copy(source, phi.at[3, rows(quarters[k])], SIDE + k, (beside, grid)).start()

    def side_relay(k):
        @pl.when(even_shares)
        def _():
            arrived(phi.at[4, rows(quarters[k])], DOWN + k)
            copy(phi.at[4, rows(quarters[k])], phi.at[3, rows(quarters[k])], SIDE + k, (beside, grid)).start()

    pass_on(0, mine_ref.at[lax.rem(grid, orbs)])
    for k, i in enumerate(order(across)):
        copy(mine_ref.at[i], phi.at[i, rows(grid)], CROSS + k, (band, across)).start()
    for k, i in enumerate(order(peer)):
        copy(mine_ref.at[i], phi.at[i, rows(grid)], PEER + k, (band, peer)).start()
    for i in range(orbs):
        phi[i, rows(grid), :] = mine_ref[i]

    mine, theirs = order(grid), order(peer)
    arrived(phi.at[mine[0], rows(peer)], PEER)
    pass_on(1, phi.at[mine[0], rows(peer)])
    fill_coulomb(n, coulomb)
    pot[...] = jnp.zeros_like(pot)

    def relay(k):
        arrived(phi.at[mine[k], rows(across)], CROSS + k)
        copy(phi.at[mine[k], rows(across)], phi.at[mine[k], rows(across)], RELAY + k, (band, peer)).start()

    side_relay(0)
    relay(0)
    pass_on(2, phi.at[mine[0], rows(across)])
    side_relay(1)
    relay(1)
    wanted = 1 - grid // 2

    @pl.when(shares)
    def _():
        arrived(phi.at[grid, rows(far)], RELAY + wanted)

    pass_on(3, phi.at[mine[0], rows(far)])
    side_relay(2)
    relay(2)
    side_relay(3)

    for k in range(1, orbs):
        arrived(phi.at[mine[k], rows(peer)], PEER + k)
    for k in range(orbs):
        @pl.when((last == 1) | (k != wanted))
        def _():
            arrived(phi.at[theirs[k], rows(far)], RELAY + k)

    @pl.when(odd_shares)
    def _():
        for k in range(4):
            arrived(phi.at[4, rows(quarters[k])], DOWN + k)

    def step(index, carry):
        @pl.when(shares & (index == 1))
        def _():
            for k in range(4):
                arrived(phi.at[3, rows(quarters[k])], SIDE + k)

        pairs = []
        for lane_half in range(2):
            number = 2 * index + lane_half
            near = number // orbs
            i = lax.rem(number, orbs)
            within = lax.rem(i + 1 - near, orbs)
            t = last * within + (1 - last) * (4 - near)
            ahead = lax.rem(band + 2 - near, groups)
            column = last * (band * orbs + within) + (1 - last) * (ahead * orbs + grid)
            weight = mask_ref[band * orbs + i, column].astype(jnp.float32)
            pairs.append((i, t, weight, (1 - last * near).astype(jnp.float32)))
        potentials(n, phi, pot, coulomb, work, left_ref, right_ref, pairs)
        return carry

    lax.fori_loop(0, orbs, step, 0)

    back = (across, far, peer, grid)
    distance = (2, 3, 1)

    @pl.when(shares)
    def _():
        for k in range(4):
            copy(pot.at[3, rows(back[k])], side.at[rows(back[k])], SIDE_BACK + k, (beside, grid)).start()

    def up_send(k):
        copy(pot.at[4, rows(back[k])], up.at[rows(back[k])], UP_BACK + k, (above, grid)).start()

    @pl.when(odd_shares)
    def _():
        for k in range(4):
            up_send(k)

    def give(i, k):
        d = distance[k]
        copy(pot.at[i, rows(back[k])], red.at[d - 1, i], REDUCE + (d - 1) * orbs + i, (band, other[d])).start()

    for k in range(3):
        for shift in (1, 2):
            give(lax.rem(grid + shift, orbs), k)

    @pl.when(last == 1)
    def _():
        for k in range(3):
            give(0, k)

    def join(k):
        @pl.when(even_shares)
        def _():
            arrived(side.at[rows(back[k])], SIDE_BACK + k)
            pot[4, rows(back[k]), :] += side[rows(back[k]), :]
            up_send(k)

    def collect(k):
        @pl.when(shares)
        def _():
            arrived(up.at[rows(back[k])], UP_BACK + k)
            pot[grid, rows(back[k]), :] += up[rows(back[k]), :]

        @pl.when(odd_shares)
        def _():
            arrived(side.at[rows(back[k])], SIDE_BACK + k)
            pot[grid, rows(back[k]), :] += side[rows(back[k]), :]

        if k < 3:
            @pl.when(shares)
            def _():
                give(grid, k)

    join(0)
    join(1)
    join(2)
    collect(0)
    join(3)
    for k in range(1, 4):
        collect(k)

    for i in range(orbs):
        for d in range(1, 4):
            arrived(red.at[d - 1, i], REDUCE + (d - 1) * orbs + i)
        out_ref[i] = (pot[i, rows(grid), :] + red[0, i]) + (red[1, i] + red[2, i])

    for number in (*range(PEER, DOWN), *range(REDUCE, COPIES)):
        left_here(out_ref.at[0], number)

    @pl.when(shares)
    def _():
        for number in range(DOWN, REDUCE):
            left_here(out_ref.at[0], number)


def local(groups, orbitals, pair_mask):
    orbs, planes, cells = orbitals.shape
    n = math.isqrt(cells)
    left, right = transform_tables(n)
    in_vmem = pl.BlockSpec(memory_space=pltpu.VMEM)
    cube = (n, cells)
    return pl.pallas_call(
        functools.partial(kernel, groups),
        out_shape=jax.ShapeDtypeStruct(orbitals.shape, jnp.float32),
        in_specs=[pl.BlockSpec(memory_space=pltpu.SMEM), in_vmem, in_vmem, in_vmem],
        out_specs=in_vmem,
        scratch_shapes=[
            pltpu.VMEM((orbs + 2, *cube), jnp.float32),
            pltpu.VMEM((orbs + 2, *cube), jnp.float32),
            pltpu.VMEM((n * n, 2 * n), jnp.float32),
            pltpu.VMEM((n * (n + SKEW), 2 * n), jnp.float32),
            pltpu.VMEM(cube, jnp.float32),
            pltpu.VMEM(cube, jnp.float32),
            pltpu.VMEM((3, orbs, planes, cells), jnp.float32),
            pltpu.SemaphoreType.DMA((COPIES,)),
            pltpu.SemaphoreType.DMA((COPIES,)),
        ],
        compiler_params=pltpu.CompilerParams(
            collective_id=0, has_side_effects=True, vmem_limit_bytes=48 * 2**20),
    )(pair_mask, orbitals, left, right)


def solution(mesh):
    groups, parts = mesh.shape["band"], mesh.shape["grid"]
    assert parts == 4 and groups % 2 == 0 and groups >= 4
    return jax.shard_map(
        functools.partial(local, groups),
        mesh=mesh,
        in_specs=(P("band", "grid", None), P()),
        out_specs=P("band", "grid", None),
        check_vma=False,
    )
```

```python
import functools
import math

import jax
import jax.numpy as jnp
import numpy as np
from jax import lax
from jax.experimental import pallas as pl
from jax.experimental.pallas import tpu as pltpu
from jax.sharding import PartitionSpec as P

MESH = pl.DeviceIdType.MESH
MIXING = 0.25
BOX_LENGTH = 16.0
SKEW = 4

CHUNKS = 2

PEER = 0
CROSS = PEER + 3
RELAY = CROSS + 3 * CHUNKS
DOWN = RELAY + 3 * CHUNKS
SIDE = DOWN + 4 * CHUNKS
SIDE_BACK = SIDE + 4 * CHUNKS
UP_BACK = SIDE_BACK + 4 * CHUNKS
JOINT = UP_BACK + 4 * CHUNKS
COMB = JOINT + 3
FROM_PEER = COMB + 2
FROM_CHIP = FROM_PEER + 3 * CHUNKS
FAR = FROM_CHIP + 3 * CHUNKS
COPIES = FAR + CHUNKS


def transform_tables(n):
    ids = np.arange(n)
    angles = (ids[:, None] * ids[None, :] % n) * (2.0 * np.pi / n)
    cas = np.cos(angles) + np.sin(angles)
    high = cas.astype(jnp.bfloat16).astype(np.float64)
    low = cas - high
    none = np.zeros_like(high)
    left = np.block([[high, high], [low, none]])
    both = lambda m: np.block([[m, none], [none, m]])
    right = np.block([[both(high), both(low)], [both(high), np.zeros((2 * n, 2 * n))]])
    return jnp.asarray(left, jnp.bfloat16), jnp.asarray(right, jnp.bfloat16)


def split(values, axis):
    high = values.astype(jnp.bfloat16)
    low = (values - high.astype(jnp.float32)).astype(jnp.bfloat16)
    return jnp.concatenate([high, low], axis=axis)


def left_product(left, values):
    both = jnp.dot(left, split(values, 0), preferred_element_type=jnp.float32)
    half = both.shape[0] // 2
    return both[:half] + both[half:]


def right_product(values, right):
    both = jnp.dot(split(values, 1), right, preferred_element_type=jnp.float32)
    half = both.shape[1] // 2
    return both[:, :half] + both[:, half:]


def fill_coulomb(n, coulomb):
    lanes = 2 * n
    scale = -MIXING * BOX_LENGTH * BOX_LENGTH / math.pi / float(n**3)
    group = 4

    def signed(index):
        return jnp.where(index < n // 2, index, index - n)

    def body(step, carry):
        fy = signed(lax.broadcasted_iota(jnp.int32, (n, lanes), 0))
        fz = signed(lax.broadcasted_iota(jnp.int32, (n, lanes), 1) % n)
        plane = fy * fy + fz * fz
        for u in range(group):
            kx = step * group + u
            fx = signed(kx)
            squared = fx * fx + plane
            safe = jnp.maximum(squared, 1).astype(jnp.float32)
            coulomb[pl.ds(pl.multiple_of(kx * n, n), n), :] = jnp.where(squared > 0, scale / safe, 0.0)
        return carry

    lax.fori_loop(0, n // group, body, 0)


def densities(n, planes, phi, work, right_ref, quarter, pairs):
    lanes, half, stride = 2 * n, n // 2, n + SKEW
    (ia, ta, wa), (ib, tb, wb) = pairs
    start = quarter * planes
    rows = pl.ds(pl.multiple_of(start, planes), planes)
    lower = lax.broadcasted_iota(jnp.int32, (planes, lanes), 1) < n
    right = right_ref[...]
    block = half // 2
    for first_col in range(0, half, block):
        strips = []
        for c in range(first_col, first_col + block):
            cols = slice(c * lanes, (c + 1) * lanes)
            first = phi[ia, rows, cols] * phi[ta, rows, cols] * wa
            second = phi[ib, rows, cols] * phi[tb, rows, cols] * wb
            turned = pltpu.roll(jnp.where(lower, second, first), n, 1)
            strips += [jnp.where(lower, first, turned), jnp.where(lower, turned, second)]
        along_z = right_product(jnp.concatenate(strips, axis=0), right)
        for u in range(2 * block):
            y = 2 * first_col + u
            work[pl.ds(y * stride + start, planes), :] = along_z[u * planes:(u + 1) * planes]


def along_y(n, planes, work, left_ref, quarter):
    stride = n + SKEW
    left = left_ref[...]
    for u in range(planes // 2):
        here = [pl.ds(quarter * planes + 2 * u + j, n, stride=stride) for j in range(2)]
        done = left_product(left, jnp.concatenate([work[h, :] for h in here], axis=1))
        work[here[0], :] = done[:, :2 * n]
        work[here[1], :] = done[:, 2 * n:]


def along_x(n, work, coulomb, left_ref):
    stride = n + SKEW
    left = left_ref[...]
    for u in range(n // 2):
        here = [pl.ds((2 * u + j) * stride, n) for j in range(2)]
        factor = [coulomb[(2 * u + j) * n:(2 * u + j + 1) * n, :] for j in range(2)]
        spectrum = left_product(left, jnp.concatenate([work[h, :] for h in here], axis=1))
        done = left_product(left, spectrum * jnp.concatenate(factor, axis=1))
        work[here[0], :] = done[:, :2 * n]
        work[here[1], :] = done[:, 2 * n:]


def exchange_terms(n, planes, phi, pot, work, right_ref, quarter, last, partners):
    lanes, half, stride = 2 * n, n // 2, n + SKEW
    start = quarter * planes
    rows = pl.ds(pl.multiple_of(start, planes), planes)
    lower = lax.broadcasted_iota(jnp.int32, (planes, lanes), 1) < n
    right = right_ref[...]
    within = last.astype(jnp.float32)
    block = half // 4
    for first_col in range(0, half, block):
        solved = []
        for p in range(3):
            strips = [work[p, pl.ds(y * stride + start, planes), :]
                      for y in range(2 * first_col, 2 * (first_col + block))]
            solved.append(right_product(jnp.concatenate(strips, axis=0), right))
        for u in range(block):
            cols = slice((first_col + u) * lanes, (first_col + u + 1) * lanes)
            values = []
            for along_z in solved:
                even = along_z[2 * u * planes:(2 * u + 1) * planes]
                odd = along_z[(2 * u + 1) * planes:(2 * u + 2) * planes]
                turned = pltpu.roll(jnp.where(lower, odd, even), n, 1)
                values += [jnp.where(lower, even, turned), jnp.where(lower, turned, odd)]
            away, near = values[:3], values[3:]
            own = [phi[i, rows, cols] for i in range(3)]
            for i in range(3):
                before = (i + 2) % 3
                pot[i, rows, cols] = (away[i] * phi[partners[0][i], rows, cols]
                                      + near[i] * phi[partners[1][i], rows, cols]
                                      + away[before] * own[before] * within)
            pot[3, rows, cols] = near[0] * own[0] + near[1] * own[1] + near[2] * own[2]
            pot[4, rows, cols] = away[0] * own[0] + away[1] * own[1] + away[2] * own[2]


def kernel(groups, mask_hbm, mine_ref, left_hbm, right_hbm, out_ref,
           phi, pot, coulomb, work, side, up, comb, joint, from_peer, from_chip,
           left_ref, right_ref, mask_ref, load_sem, send_sem, recv_sem):
    orbs, planes, cells = mine_ref.shape
    n = phi.shape[1]
    depth = planes // CHUNKS
    band, grid = lax.axis_index("band"), lax.axis_index("grid")
    last = grid // orbs
    odd_band = lax.rem(band, 2)
    below, above = lax.rem(band + groups - 2, groups), lax.rem(band + 2, groups)
    beside = band + 1 - 2 * odd_band
    peer, across, far = grid + 1 - 2 * lax.rem(grid, 2), lax.rem(grid + 2, 4), 3 - grid
    shares, peer_shares = grid < orbs, peer < orbs
    even_shares = shares & (odd_band == 0)
    odd_shares = shares & (odd_band == 1)

    def order(device):
        first = device - device // orbs
        second = 1 - (device + 2) // orbs
        return first, second, orbs - first - second

    def rows(quarter):
        return pl.ds(pl.multiple_of(quarter * planes, planes), planes)

    def part(quarter, c):
        return pl.ds(pl.multiple_of(quarter * planes + c * depth, depth), depth)

    def copy(source, target, number, device, sent=None):
        return pltpu.make_async_remote_copy(
            src_ref=source, dst_ref=target, send_sem=send_sem.at[number if sent is None else sent],
            recv_sem=recv_sem.at[number], device_id=device, device_id_type=MESH)

    def arrived(target, number):
        copy(target, target, number, (band, peer)).wait_recv()

    def gone(target, number):
        copy(target, target, number, (band, peer)).wait_send()

    loads = [pltpu.make_async_copy(mine_ref.at[i], phi.at[i, rows(grid)], load_sem.at[i]) for i in range(orbs)]
    loads += [pltpu.make_async_copy(a, b, load_sem.at[orbs + k]) for k, (a, b) in enumerate(
        ((mask_hbm, mask_ref), (left_hbm, left_ref), (right_hbm, right_ref)))]
    for load in loads:
        load.start()

    barrier = pltpu.get_barrier_semaphore()
    for device in ((band, peer), (band, across), (band, far), (beside, grid), (below, grid), (above, grid)):
        pl.semaphore_signal(barrier, inc=1, device_id=device, device_id_type=MESH)
    for load in loads[:orbs]:
        load.wait()
    pl.semaphore_wait(barrier, 6)

    quarters = (grid, peer, across, far)

    def pass_on(k, c):
        piece = phi.at[lax.rem(grid, orbs), part(quarters[k], c)]

        @pl.when(shares)
        def _():
            copy(piece, phi.at[4, part(quarters[k], c)], DOWN + k * CHUNKS + c, (below, grid)).start()

        @pl.when(odd_shares)
        def _():
            copy(piece, phi.at[3, part(quarters[k], c)], SIDE + k * CHUNKS + c, (beside, grid)).start()

    def side_relay(m):
        k, c = divmod(m, CHUNKS)
        piece = phi.at[4, part(quarters[k], c)]

        @pl.when(even_shares)
        def _():
            arrived(piece, DOWN + m)
            copy(piece, phi.at[3, part(quarters[k], c)], SIDE + m, (beside, grid)).start()

    for c in range(CHUNKS):
        pass_on(0, c)
    for k, i in enumerate(order(across)):
        for c in range(CHUNKS):
            piece = phi.at[i, part(grid, c)]
            copy(piece, piece, CROSS + k * CHUNKS + c, (band, across)).start()
    for k, i in enumerate(order(peer)):
        piece = phi.at[i, rows(grid)]
        copy(piece, piece, PEER + k, (band, peer)).start()

    mine, theirs = order(grid), order(peer)
    arrived(phi.at[mine[0], rows(peer)], PEER)
    for c in range(CHUNKS):
        pass_on(1, c)
    fill_coulomb(n, coulomb)
    for load in loads[orbs:]:
        load.wait()

    def relay(k, c):
        piece = phi.at[mine[k], part(across, c)]
        arrived(piece, CROSS + k * CHUNKS + c)
        copy(piece, piece, RELAY + k * CHUNKS + c, (band, peer)).start()

    wanted = 1 - grid // 2

    def far_on(c):
        @pl.when(shares)
        def _():
            arrived(phi.at[grid, part(far, c)], RELAY + wanted * CHUNKS + c)

        pass_on(3, c)

    def partner(i, near):
        within = lax.rem(i + 1 - near, orbs)
        return last * within + (1 - last) * (4 - near)

    def forward(p, quarter):
        pairs = []
        for lane_half in range(2):
            number = 2 * p + lane_half
            near, i = number // orbs, lax.rem(number, orbs)
            ahead = lax.rem(band + 2 - near, groups)
            column = last * (band * orbs + lax.rem(i + 1 - near, orbs)) + (1 - last) * (ahead * orbs + grid)
            weight = mask_ref[band * orbs + i, column].astype(jnp.float32)
            pairs.append((i, partner(i, near), weight))
        densities(n, planes, phi, work.at[p], right_ref, quarter, pairs)
        along_y(n, planes, work.at[p], left_ref, quarter)

    def forward_rest(quarter):
        def body(p, carry):
            forward(p, quarter)
            return carry

        lax.fori_loop(1, 3, body, 0)

    def await_down(k):
        @pl.when(odd_shares)
        def _():
            for c in range(CHUNKS):
                arrived(phi.at[4, part(quarters[k], c)], DOWN + k * CHUNKS + c)

    def await_side(k):
        @pl.when(shares)
        def _():
            for c in range(CHUNKS):
                arrived(phi.at[3, part(quarters[k], c)], SIDE + k * CHUNKS + c)

    zero = lax.rem(grid, 1)
    for c in range(CHUNKS):
        relay(0, c)
        pass_on(2, c)
        side_relay(c)
    await_down(0)
    forward(zero, quarters[0])
    for c in range(CHUNKS):
        relay(1, c)
        side_relay(CHUNKS + c)
        far_on(c)
    await_down(1)
    for k in range(1, orbs):
        arrived(phi.at[mine[k], rows(peer)], PEER + k)
    forward(zero, quarters[1])
    for c in range(CHUNKS):
        side_relay(2 * CHUNKS + c)
        relay(2, c)
    await_down(2)
    forward(zero, quarters[2])
    for c in range(CHUNKS - 1):
        side_relay(3 * CHUNKS + c)
    for k in range(2):
        await_side(k)
        forward_rest(quarters[k])
    side_relay(4 * CHUNKS - 1)
    for k in range(orbs):
        @pl.when((last == 1) | (k != wanted))
        def _():
            for c in range(CHUNKS):
                arrived(phi.at[theirs[k], part(far, c)], RELAY + k * CHUNKS + c)
    await_down(3)
    forward(zero, quarters[3])

    def solve(p, carry):
        @pl.when(p == 1)
        def _():
            for k in (2, 3):
                await_side(k)
                forward_rest(quarters[k])

        along_x(n, work.at[p], coulomb, left_ref)
        return carry

    lax.fori_loop(0, 3, solve, 0)

    back = (across, far, peer, grid)
    partners = [[partner(i, near) for i in range(3)] for near in range(2)]

    def up_send(m):
        k, c = divmod(m, CHUNKS)
        copy(pot.at[4, part(back[k], c)], up.at[part(back[k], c)], UP_BACK + m, (above, grid)).start()

    def elsewhere(i):
        return grid // 2 != i // 2

    for k in range(4):
        def inverse(p, carry):
            along_y(n, planes, work.at[p], left_ref, back[k])
            return carry

        lax.fori_loop(0, 3, inverse, 0)
        exchange_terms(n, planes, phi, pot, work, right_ref, back[k], last, partners)

        @pl.when(shares)
        def _():
            for c in range(CHUNKS):
                here = part(back[k], c)
                copy(pot.at[3, here], side.at[here], SIDE_BACK + k * CHUNKS + c, (beside, grid)).start()

        @pl.when(odd_shares)
        def _():
            for c in range(CHUNKS):
                up_send(k * CHUNKS + c)

        if k == 1:
            for i in range(orbs):
                @pl.when(elsewhere(i))
                def _():
                    copy(pot.at[i, rows(far)], joint.at[i], JOINT + i, (band, peer)).start()

        if k < 2:
            @pl.when(peer_shares)
            def _():
                copy(pot.at[peer, rows(back[k])], comb.at[1 - k], COMB + 1 - k, (band, peer)).start()

        if k == 2:
            for i in range(orbs):
                @pl.when(elsewhere(i) | (peer == i))
                def _():
                    for c in range(CHUNKS):
                        copy(pot.at[i, part(peer, c)], from_peer.at[i, pl.ds(c * depth, depth)],
                             FROM_PEER + i * CHUNKS + c, (band, peer)).start()

    for i in range(orbs):
        @pl.when(elsewhere(i))
        def _():
            arrived(joint.at[i], JOINT + i)
            pot[i, rows(across), :] += joint[i]
            for c in range(CHUNKS):
                copy(pot.at[i, part(across, c)], from_chip.at[i, pl.ds(c * depth, depth)],
                     FROM_CHIP + i * CHUNKS + c, (band, across)).start()

    def join(m):
        k, c = divmod(m, CHUNKS)

        @pl.when(even_shares)
        def _():
            arrived(side.at[part(back[k], c)], SIDE_BACK + m)
            pot[4, part(back[k], c), :] += side[part(back[k], c), :]
            up_send(m)

    def collect(m):
        k, c = divmod(m, CHUNKS)
        here = part(back[k], c)
        inner = pl.ds(c * depth, depth)

        @pl.when(shares)
        def _():
            if k < 2 and c == 0:
                arrived(comb.at[k], COMB + k)
            arrived(up.at[here], UP_BACK + m)
            if k < 2:
                pot[grid, here, :] += up[here, :] + comb[k, inner, :]
            else:
                pot[grid, here, :] += up[here, :]

        @pl.when(odd_shares)
        def _():
            arrived(side.at[here], SIDE_BACK + m)
            pot[grid, here, :] += side[here, :]

        @pl.when(shares)
        def _():
            source = pot.at[grid, here]
            number = grid * CHUNKS + c
            if k == 0:
                copy(source, from_chip.at[grid, inner], FROM_CHIP + number, (band, across)).start()
            elif k == 1:
                copy(source, from_chip.at[grid, inner], FROM_CHIP + number, (band, far), FAR + c).start()
            elif k == 2:
                copy(source, from_peer.at[grid, inner], FROM_PEER + number, (band, peer)).start()

    join(0)
    join(1)
    for m in range(4 * CHUNKS):
        collect(m)
        if m + 2 < 4 * CHUNKS:
            join(m + 2)

    for i in range(orbs):
        for c in range(CHUNKS):
            inner = pl.ds(c * depth, depth)
            arrived(from_peer.at[i, inner], FROM_PEER + i * CHUNKS + c)
            arrived(from_chip.at[i, inner], FROM_CHIP + i * CHUNKS + c)
        out_ref[i] = pot[i, rows(grid), :] + from_peer[i] + from_chip[i]

    whole, chunk = comb.at[0], comb.at[0, pl.ds(0, depth)]
    for number in range(PEER, PEER + 3):
        gone(whole, number)
    for number in range(CROSS, DOWN):
        gone(chunk, number)

    @pl.when(shares)
    def _():
        for number in (*range(DOWN, JOINT), *range(FAR, FAR + CHUNKS)):
            gone(chunk, number)
        for c in range(CHUNKS):
            gone(chunk, FROM_CHIP + grid * CHUNKS + c)
            gone(chunk, FROM_PEER + grid * CHUNKS + c)

    @pl.when(peer_shares)
    def _():
        gone(whole, COMB)
        gone(whole, COMB + 1)
        for c in range(CHUNKS):
            gone(chunk, FROM_PEER + peer * CHUNKS + c)

    for i in range(orbs):
        @pl.when(elsewhere(i))
        def _():
            gone(whole, JOINT + i)
            for c in range(CHUNKS):
                gone(chunk, FROM_PEER + i * CHUNKS + c)
                gone(chunk, FROM_CHIP + i * CHUNKS + c)


def local(groups, orbitals, pair_mask):
    orbs, planes, cells = orbitals.shape
    n = math.isqrt(cells)
    left, right = transform_tables(n)
    in_hbm = pl.BlockSpec(memory_space=pltpu.HBM)
    cube, piece = (n, cells), (planes, cells)
    return pl.pallas_call(
        functools.partial(kernel, groups),
        out_shape=jax.ShapeDtypeStruct(orbitals.shape, jnp.float32),
        in_specs=[in_hbm] * 4,
        out_specs=pl.BlockSpec(memory_space=pltpu.VMEM),
        scratch_shapes=[
            pltpu.VMEM((orbs + 2, *cube), jnp.float32),
            pltpu.VMEM((orbs + 2, *cube), jnp.float32),
            pltpu.VMEM((n * n, 2 * n), jnp.float32),
            pltpu.VMEM((3, n * (n + SKEW), 2 * n), jnp.float32),
            pltpu.VMEM(cube, jnp.float32),
            pltpu.VMEM(cube, jnp.float32),
            pltpu.VMEM((2, *piece), jnp.float32),
            pltpu.VMEM((orbs, *piece), jnp.float32),
            pltpu.VMEM((orbs, *piece), jnp.float32),
            pltpu.VMEM((orbs, *piece), jnp.float32),
            pltpu.VMEM(left.shape, jnp.bfloat16),
            pltpu.VMEM(right.shape, jnp.bfloat16),
            pltpu.SMEM(pair_mask.shape, jnp.int32),
            pltpu.SemaphoreType.DMA((orbs + 3,)),
            pltpu.SemaphoreType.DMA((COPIES,)),
            pltpu.SemaphoreType.DMA((COPIES,)),
        ],
        compiler_params=pltpu.CompilerParams(
            collective_id=0, has_side_effects=True),
    )(pair_mask, orbitals, left, right)


def solution(mesh):
    groups, parts = mesh.shape["band"], mesh.shape["grid"]
    assert parts == 4 and groups % 2 == 0 and groups >= 4
    return jax.shard_map(
        functools.partial(local, groups),
        mesh=mesh,
        in_specs=(P("band", "grid", None), P()),
        out_specs=P("band", "grid", None),
        check_vma=False,
    )
```

```python
import functools
import math

import jax
import jax.numpy as jnp
import numpy as np
from jax import lax
from jax.experimental import pallas as pl
from jax.experimental.pallas import tpu as pltpu
from jax.sharding import PartitionSpec as P

MESH = pl.DeviceIdType.MESH
MIXING = 0.25
BOX_LENGTH = 16.0
SKEW = 4

HALVES = 2
SMALL = ((0, 0, 1), (0, 1, 1), (0, 2, 2), (0, 4, 4), (1, 0, 8))
HALF = ((0, 0, 8), (1, 0, 8))


TAIL = ((0, 0, 8), (1, 0, 4), (1, 4, 2), (1, 6, 2))


def pieces(cuts):
    return [(k, row, 1, column, parts) for k, cut in enumerate(cuts) for row, column, parts in cut]


AHEAD = BACK = pieces((SMALL, HALF, HALF, TAIL))
JOINED_BEFORE = (0, (2, 0, 1, 0, 8))


def in_order_of_arrival(cuts):
    hop, sent, free, events = 0.3, 0.0, 0.0, []
    for m, piece in enumerate(cuts):
        size = piece[4] / 16
        sent += size
        free = max(free, sent + hop) + size
        events += [(sent + hop, 0, m), (free + hop, 1, m)]
    return [(what, m) for _, what, m in sorted(events)]

PEER = 0
CROSS = PEER + 3
RELAY = CROSS + 3 * HALVES
DOWN = RELAY + 3 * HALVES
SIDE = DOWN + len(AHEAD)
SIDE_BACK = SIDE + len(AHEAD)
UP_BACK = SIDE_BACK + len(BACK)
JOINT = UP_BACK + len(BACK)
COMB = JOINT + 3
FROM_PEER = COMB + 2
FROM_CHIP = FROM_PEER + 3
FAR = FROM_CHIP + 3
COPIES = FAR + 1


def transform_tables(n):
    ids = np.arange(n)
    angles = (ids[:, None] * ids[None, :] % n) * (2.0 * np.pi / n)
    cas = np.cos(angles) + np.sin(angles)
    high = cas.astype(jnp.bfloat16).astype(np.float64)
    low = cas - high
    none = np.zeros_like(high)
    left = np.block([[high, high], [low, none]])
    both = lambda m: np.block([[m, none], [none, m]])
    right = np.block([[both(high), both(low)], [both(high), np.zeros((2 * n, 2 * n))]])
    return jnp.asarray(left, jnp.bfloat16), jnp.asarray(right, jnp.bfloat16)


def split(values, axis):
    high = values.astype(jnp.bfloat16)
    low = (values - high.astype(jnp.float32)).astype(jnp.bfloat16)
    return jnp.concatenate([high, low], axis=axis)


def left_product(left, values):
    both = jnp.dot(left, split(values, 0), preferred_element_type=jnp.float32)
    half = both.shape[0] // 2
    return both[:half] + both[half:]


def right_product(values, right):
    both = jnp.dot(split(values, 1), right, preferred_element_type=jnp.float32)
    half = both.shape[1] // 2
    return both[:, :half] + both[:, half:]


def fill_coulomb(n, coulomb):
    lanes = 2 * n
    scale = -MIXING * BOX_LENGTH * BOX_LENGTH / math.pi / float(n**3)
    group = 4

    def signed(index):
        return jnp.where(index < n // 2, index, index - n)

    def body(step, carry):
        fy = signed(lax.broadcasted_iota(jnp.int32, (n, lanes), 0))
        fz = signed(lax.broadcasted_iota(jnp.int32, (n, lanes), 1) % n)
        plane = fy * fy + fz * fz
        for u in range(group):
            kx = step * group + u
            fx = signed(kx)
            squared = fx * fx + plane
            safe = jnp.maximum(squared, 1).astype(jnp.float32)
            coulomb[pl.ds(pl.multiple_of(kx * n, n), n), :] = jnp.where(squared > 0, scale / safe, 0.0)
        return carry

    lax.fori_loop(0, n // group, body, 0)


def densities(n, planes, phi, work, right_ref, quarter, pairs):
    lanes, half, stride = 2 * n, n // 2, n + SKEW
    (ia, ta, wa), (ib, tb, wb) = pairs
    start = quarter * planes
    rows = pl.ds(pl.multiple_of(start, planes), planes)
    lower = lax.broadcasted_iota(jnp.int32, (planes, lanes), 1) < n
    right = right_ref[...]
    block = half // 2
    for first_col in range(0, half, block):
        strips = []
        for c in range(first_col, first_col + block):
            cols = slice(c * lanes, (c + 1) * lanes)
            first = phi[ia, rows, cols] * phi[ta, rows, cols] * wa
            second = phi[ib, rows, cols] * phi[tb, rows, cols] * wb
            turned = pltpu.roll(jnp.where(lower, second, first), n, 1)
            strips += [jnp.where(lower, first, turned), jnp.where(lower, turned, second)]
        along_z = right_product(jnp.concatenate(strips, axis=0), right)
        for u in range(2 * block):
            y = 2 * first_col + u
            work[pl.ds(y * stride + start, planes), :] = along_z[u * planes:(u + 1) * planes]


def along_y(n, planes, works, left_ref, quarter):
    stride = n + SKEW
    left = left_ref[...]
    for work in works:
        for u in range(planes // 2):
            here = [pl.ds(quarter * planes + 2 * u + j, n, stride=stride) for j in range(2)]
            done = left_product(left, jnp.concatenate([work[h, :] for h in here], axis=1))
            work[here[0], :] = done[:, :2 * n]
            work[here[1], :] = done[:, 2 * n:]


def along_x(n, work, coulomb, left_ref):
    stride = n + SKEW
    left = left_ref[...]
    for u in range(n // 2):
        here = [pl.ds((2 * u + j) * stride, n) for j in range(2)]
        factor = [coulomb[(2 * u + j) * n:(2 * u + j + 1) * n, :] for j in range(2)]
        spectrum = left_product(left, jnp.concatenate([work[h, :] for h in here], axis=1))
        done = left_product(left, spectrum * jnp.concatenate(factor, axis=1))
        work[here[0], :] = done[:, :2 * n]
        work[here[1], :] = done[:, 2 * n:]


def exchange_terms(n, planes, phi, pot, work, right_ref, quarter, last, partners):
    lanes, half, stride = 2 * n, n // 2, n + SKEW
    start = quarter * planes
    rows = pl.ds(pl.multiple_of(start, planes), planes)
    lower = lax.broadcasted_iota(jnp.int32, (planes, lanes), 1) < n
    right = right_ref[...]
    within = last.astype(jnp.float32)
    block = half // 4
    for first_col in range(0, half, block):
        solved = []
        for p in range(3):
            strips = [work[p, pl.ds(y * stride + start, planes), :]
                      for y in range(2 * first_col, 2 * (first_col + block))]
            solved.append(right_product(jnp.concatenate(strips, axis=0), right))
        for u in range(block):
            cols = slice((first_col + u) * lanes, (first_col + u + 1) * lanes)
            values = []
            for along_z in solved:
                even = along_z[2 * u * planes:(2 * u + 1) * planes]
                odd = along_z[(2 * u + 1) * planes:(2 * u + 2) * planes]
                turned = pltpu.roll(jnp.where(lower, odd, even), n, 1)
                values += [jnp.where(lower, even, turned), jnp.where(lower, turned, odd)]
            away, near = values[:3], values[3:]
            own = [phi[i, rows, cols] for i in range(3)]
            for i in range(3):
                before = (i + 2) % 3
                pot[i, rows, cols] = (away[i] * phi[partners[0][i], rows, cols]
                                      + near[i] * phi[partners[1][i], rows, cols]
                                      + away[before] * own[before] * within)
            pot[3, rows, cols] = near[0] * own[0] + near[1] * own[1] + near[2] * own[2]
            pot[4, rows, cols] = away[0] * own[0] + away[1] * own[1] + away[2] * own[2]


def kernel(groups, mask_hbm, mine_ref, left_hbm, right_hbm, out_ref,
           phi, pot, coulomb, work, side, up, comb, joint, from_peer, from_chip, result,
           left_ref, right_ref, mask_ref, load_sem, send_sem, recv_sem):
    orbs, planes, cells = mine_ref.shape
    n = phi.shape[1]
    band, grid = lax.axis_index("band"), lax.axis_index("grid")
    last = grid // orbs
    odd_band = lax.rem(band, 2)
    below, above = lax.rem(band + groups - 2, groups), lax.rem(band + 2, groups)
    beside = band + 1 - 2 * odd_band
    peer, across, far = grid + 1 - 2 * lax.rem(grid, 2), lax.rem(grid + 2, 4), 3 - grid
    shares, peer_shares = grid < orbs, peer < orbs
    even_shares = shares & (odd_band == 0)
    odd_shares = shares & (odd_band == 1)

    def order(device):
        first, second = 2 * (device // 2), 1 - device // 2
        return first, second, orbs - first - second

    def rows(quarter):
        return pl.ds(pl.multiple_of(quarter * planes, planes), planes)

    depth, width = planes // 2, cells // 8

    def inner(piece):
        _, row, halves, column, parts = piece
        return pl.ds(row * depth, halves * depth), pl.ds(column * width, parts * width)

    def part(quarter, piece):
        _, row, halves, column, parts = piece
        first = pl.multiple_of(quarter * planes + row * depth, depth)
        return pl.ds(first, halves * depth), pl.ds(column * width, parts * width)

    def half(quarter, c):
        return pl.ds(pl.multiple_of(quarter * planes + c * depth, depth), depth)

    def copy(source, target, number, device, sent=None):
        return pltpu.make_async_remote_copy(
            src_ref=source, dst_ref=target, send_sem=send_sem.at[number if sent is None else sent],
            recv_sem=recv_sem.at[number], device_id=device, device_id_type=MESH)

    def arrived(target, number):
        copy(target, target, number, (band, peer)).wait_recv()

    def gone(target, number):
        copy(target, target, number, (band, peer)).wait_send()

    loads = [pltpu.make_async_copy(mine_ref.at[i], phi.at[i, rows(grid)], load_sem.at[i]) for i in range(orbs)]
    loads += [pltpu.make_async_copy(a, b, load_sem.at[orbs + k]) for k, (a, b) in enumerate(
        ((mask_hbm, mask_ref), (left_hbm, left_ref), (right_hbm, right_ref)))]
    for load in loads:
        load.start()

    barrier = pltpu.get_barrier_semaphore()
    for device in ((band, peer), (band, across), (band, far), (beside, grid), (below, grid), (above, grid)):
        pl.semaphore_signal(barrier, inc=1, device_id=device, device_id_type=MESH)
    for load in loads[:orbs]:
        load.wait()
    pl.semaphore_wait(barrier, 6)

    quarters = (grid, peer, across, far)

    def pass_on(k, only=None):
        for m, piece in enumerate(AHEAD):
            if piece[0] != k or only not in (None, piece[1]):
                continue
            here = part(quarters[k], piece)
            source = phi.at[lax.rem(grid, orbs), *here]

            @pl.when(shares)
            def _():
                copy(source, phi.at[4, *here], DOWN + m, (below, grid)).start()

            @pl.when(odd_shares)
            def _():
                copy(source, phi.at[3, *here], SIDE + m, (beside, grid)).start()

    def side_relay(m):
        here = part(quarters[AHEAD[m][0]], AHEAD[m])

        @pl.when(even_shares)
        def _():
            arrived(phi.at[4, *here], DOWN + m)
            copy(phi.at[4, *here], phi.at[3, *here], SIDE + m, (beside, grid)).start()

    def side_relays(k):
        return [m for m, piece in enumerate(AHEAD) if piece[0] == k]

    first_turn, second_turn = grid != 1, grid == 1
    pl.when(first_turn)(lambda: pass_on(0))
    for k, i in enumerate(order(across)):
        for c in range(HALVES):
            piece = phi.at[i, half(grid, c)]
            copy(piece, piece, CROSS + k * HALVES + c, (band, across)).start()
    for k, i in enumerate(order(peer)):
        piece = phi.at[i, rows(grid)]
        copy(piece, piece, PEER + k, (band, peer)).start()

    mine, theirs = order(grid), order(peer)
    for k in range(orbs):
        arrived(phi.at[mine[k], rows(peer)], PEER + k)
    pl.when(first_turn)(lambda: pass_on(1))
    fill_coulomb(n, coulomb)
    for load in loads[orbs:]:
        load.wait()

    def relay(k, c):
        piece = phi.at[mine[k], half(across, c)]
        arrived(piece, CROSS + k * HALVES + c)
        copy(piece, piece, RELAY + k * HALVES + c, (band, peer)).start()

    wanted = lax.rem(grid, 2)

    def far_on(c):
        @pl.when(shares)
        def _():
            arrived(phi.at[grid, half(far, c)], RELAY + wanted * HALVES + c)

        pass_on(3, c)

    def partner(i, near):
        within = lax.rem(i + 1 - near, orbs)
        return last * within + (1 - last) * (4 - near)

    def density(p, quarter):
        pairs = []
        for lane_half in range(2):
            number = 2 * p + lane_half
            near, i = number // orbs, lax.rem(number, orbs)
            ahead = lax.rem(band + 2 - near, groups)
            column = last * (band * orbs + lax.rem(i + 1 - near, orbs)) + (1 - last) * (ahead * orbs + grid)
            weight = mask_ref[band * orbs + i, column].astype(jnp.float32)
            pairs.append((i, partner(i, near), weight))
        densities(n, planes, phi, work.at[p], right_ref, quarter, pairs)

    def await_down(k):
        @pl.when(odd_shares)
        def _():
            for m in side_relays(k):
                arrived(phi.at[4, *part(quarters[k], AHEAD[m])], DOWN + m)

    def await_side(k):
        @pl.when(shares)
        def _():
            for m in side_relays(k):
                arrived(phi.at[3, *part(quarters[k], AHEAD[m])], SIDE + m)

    def choose(index, values):
        chosen = values[0]
        for position, value in enumerate(values[1:], 1):
            chosen = jnp.where(index == position, value, chosen)
        return chosen

    def relayed(k, rows_only=None):
        for m in side_relays(k):
            if rows_only in (None, AHEAD[m][1]):
                side_relay(m)

    def all_relayed():
        for k in range(orbs):
            @pl.when((last == 1) | (k != wanted))
            def _():
                for c in range(HALVES):
                    arrived(phi.at[theirs[k], half(far, c)], RELAY + k * HALVES + c)

    def early_0():
        relayed(0, 0)
        relay(0, 0)
        pass_on(2, 0)
        relayed(0, 1)
        far_on(0)
        await_down(0)

    def early_1():
        relayed(1, 0)
        relay(0, 1)
        pass_on(2, 1)
        relayed(1, 1)
        far_on(1)
        await_down(1)

    def early_2():
        relayed(2, 0)
        await_side(0)

    def early_3():
        relayed(2, 1)
        relay(1, 0)
        await_side(1)

    def early_4():
        relayed(3)
        relay(1, 1)
        relay(2, 0)
        relay(2, 1)
        await_down(2)

    def early_6():
        all_relayed()
        await_down(3)

    def late_0():
        for k in range(2):
            for c in range(HALVES):
                relay(k, c)
        for k in range(3):
            pass_on(k)
        relayed(0, 0)
        relay(2, 0)
        far_on(0)
        far_on(1)
        relayed(0, 1)
        relay(2, 1)
        await_down(0)

    def late_1():
        relayed(1)
        await_down(1)

    def late_3():
        relayed(2)
        await_side(1)

    def late_5():
        relayed(3, 0)
        await_side(2)

    def late_6():
        relayed(3, 1)
        all_relayed()
        await_down(3)

    first_work, other_works, along = range(3)
    steps = ((first_work, 0), (first_work, 1), (other_works, 0), (other_works, 1), (first_work, 2),
             (other_works, 2), (first_work, 3), (along, 0), (other_works, 3), (along, 1), (along, 2))
    early = {0: early_0, 1: early_1, 2: early_2, 3: early_3, 4: early_4, 5: lambda: await_side(2), 6: early_6}
    late = {0: late_0, 1: late_1, 2: lambda: await_side(0), 3: late_3, 4: lambda: await_down(2),
            5: late_5, 6: late_6}

    def step(index, carry):
        for turn, actions in ((first_turn, early), (second_turn, late)):
            for position, action in actions.items():
                pl.when(turn & (index == position))(action)
        pl.when(index == 8)(lambda: await_side(3))
        kind = choose(index, [which for which, _ in steps])
        number = choose(index, [k for _, k in steps])
        quarter = choose(number, quarters)

        @pl.when(kind == first_work)
        def _():
            density(0, quarter)
            along_y(n, planes, [work.at[0]], left_ref, quarter)

        @pl.when(kind == other_works)
        def _():
            density(1, quarter)
            density(2, quarter)
            along_y(n, planes, [work.at[1], work.at[2]], left_ref, quarter)

        @pl.when(kind == along)
        def _():
            along_x(n, work.at[number], coulomb, left_ref)

        return carry

    lax.fori_loop(0, len(steps), step, 0)

    back = (across, far, peer, grid)
    partners = [[partner(i, near) for i in range(3)] for near in range(2)]

    def up_send(m):
        here = part(back[BACK[m][0]], BACK[m])
        copy(pot.at[4, *here], up.at[*here], UP_BACK + m, (above, grid)).start()

    def elsewhere(i):
        return grid // 2 != i // 2

    def send_back(k):
        @pl.when(shares)
        def _():
            for m, piece in enumerate(BACK):
                if piece[0] == k:
                    here = part(back[k], piece)
                    copy(pot.at[3, *here], side.at[*here], SIDE_BACK + m, (beside, grid)).start()

        @pl.when(odd_shares)
        def _():
            for m, piece in enumerate(BACK):
                if piece[0] == k:
                    up_send(m)

        if k == 1:
            for i in range(orbs):
                @pl.when(elsewhere(i))
                def _():
                    copy(pot.at[i, rows(far)], joint.at[i], JOINT + i, (band, peer)).start()

        if k < 2:
            @pl.when(peer_shares)
            def _():
                copy(pot.at[peer, rows(back[k])], comb.at[1 - k], COMB + 1 - k, (band, peer)).start()

        if k == 2:
            for i in range(orbs):
                @pl.when(elsewhere(i) | (peer == i))
                def _():
                    copy(pot.at[i, rows(peer)], from_peer.at[i], FROM_PEER + i, (band, peer)).start()

    def back_step(index, carry):
        quarter = choose(index, back)

        along_y(n, planes, [work.at[p] for p in range(3)], left_ref, quarter)
        exchange_terms(n, planes, phi, pot, work, right_ref, quarter, last, partners)
        for k in range(4):
            pl.when(index == k)(functools.partial(send_back, k))
        return carry

    lax.fori_loop(0, 4, back_step, 0)

    def join(m):
        here = part(back[BACK[m][0]], BACK[m])

        @pl.when(even_shares)
        def _():
            arrived(side.at[*here], SIDE_BACK + m)
            pot[4, *here] += side[*here]
            up_send(m)

    def collect(m):
        k = BACK[m][0]
        here, within = part(back[k], BACK[m]), inner(BACK[m])

        @pl.when(shares)
        def _():
            if k < 2 and BACK[m - 1][0] != k:
                arrived(comb.at[k], COMB + k)
            arrived(up.at[*here], UP_BACK + m)
            if k < 2:
                pot[grid, *here] += up[*here] + comb[k, *within]
            else:
                pot[grid, *here] += up[*here]

        @pl.when(odd_shares)
        def _():
            arrived(side.at[*here], SIDE_BACK + m)
            pot[grid, *here] += side[*here]

        @pl.when(shares)
        def _():
            source = pot.at[grid, *here]
            if k == 0:
                copy(source, from_chip.at[grid, *within], FROM_CHIP + grid, (band, across)).start()
            elif k == 1:
                copy(source, from_chip.at[grid, *within], FROM_CHIP + grid, (band, far), FAR).start()
            elif k == 2:
                copy(source, from_peer.at[grid, *within], FROM_PEER + grid, (band, peer)).start()

    def finish(i, k):
        arrived(from_peer.at[i], FROM_PEER + i)
        arrived(from_chip.at[i], FROM_CHIP + i)
        result[i] = pot[i, rows(grid), :] + from_peer[i] + from_chip[i]
        pltpu.make_async_copy(result.at[i], out_ref.at[i], load_sem.at[k]).start()

    def joined():
        for i in range(orbs):
            @pl.when(elsewhere(i))
            def _():
                arrived(joint.at[i], JOINT + i)
                pot[i, rows(across), :] += joint[i]
                copy(pot.at[i, rows(across)], from_chip.at[i], FROM_CHIP + i, (band, across)).start()

    for what, m in in_order_of_arrival(BACK):
        if (what, BACK[m]) == JOINED_BEFORE:
            joined()
        (collect if what else join)(m)
    soon = choose(grid, (2, 2, 0, 0))
    own = choose(grid, (0, 1, 2, 2))
    for k, i in enumerate((soon, orbs - soon - own, own)):
        finish(i, k)

    whole, halved = comb.at[0], comb.at[0, pl.ds(0, planes // HALVES)]
    for number in range(PEER, PEER + 3):
        gone(whole, number)
    for number in range(CROSS, DOWN):
        gone(halved, number)

    @pl.when(shares)
    def _():
        for first, cuts in ((DOWN, AHEAD), (SIDE, AHEAD), (SIDE_BACK, BACK), (UP_BACK, BACK)):
            for m, piece in enumerate(cuts):
                gone(comb.at[0, *inner(piece)], first + m)
        for number in (FROM_CHIP + grid, FROM_PEER + grid, FAR):
            gone(whole, number)

    @pl.when(peer_shares)
    def _():
        for number in (COMB, COMB + 1, FROM_PEER + peer):
            gone(whole, number)

    for i in range(orbs):
        @pl.when(elsewhere(i))
        def _():
            for number in (JOINT + i, FROM_PEER + i, FROM_CHIP + i):
                gone(whole, number)

    for k in range(orbs):
        pltpu.make_async_copy(result.at[k], out_ref.at[k], load_sem.at[k]).wait()


def local(groups, orbitals, pair_mask):
    orbs, planes, cells = orbitals.shape
    n = math.isqrt(cells)
    left, right = transform_tables(n)
    in_hbm = pl.BlockSpec(memory_space=pltpu.HBM)
    cube, piece = (n, cells), (planes, cells)
    return pl.pallas_call(
        functools.partial(kernel, groups),
        out_shape=jax.ShapeDtypeStruct(orbitals.shape, jnp.float32),
        in_specs=[in_hbm] * 4,
        out_specs=in_hbm,
        scratch_shapes=[
            pltpu.VMEM((orbs + 2, *cube), jnp.float32),
            pltpu.VMEM((orbs + 2, *cube), jnp.float32),
            pltpu.VMEM((n * n, 2 * n), jnp.float32),
            pltpu.VMEM((3, n * (n + SKEW), 2 * n), jnp.float32),
            pltpu.VMEM(cube, jnp.float32),
            pltpu.VMEM(cube, jnp.float32),
            pltpu.VMEM((2, *piece), jnp.float32),
            pltpu.VMEM((orbs, *piece), jnp.float32),
            pltpu.VMEM((orbs, *piece), jnp.float32),
            pltpu.VMEM((orbs, *piece), jnp.float32),
            pltpu.VMEM((orbs, *piece), jnp.float32),
            pltpu.VMEM(left.shape, jnp.bfloat16),
            pltpu.VMEM(right.shape, jnp.bfloat16),
            pltpu.SMEM(pair_mask.shape, jnp.int32),
            pltpu.SemaphoreType.DMA((orbs + 3,)),
            pltpu.SemaphoreType.DMA((COPIES,)),
            pltpu.SemaphoreType.DMA((COPIES,)),
        ],
        compiler_params=pltpu.CompilerParams(
            collective_id=0, has_side_effects=True),
    )(pair_mask, orbitals, left, right)


def solution(mesh):
    groups, parts = mesh.shape["band"], mesh.shape["grid"]
    assert parts == 4 and groups % 2 == 0 and groups >= 4
    return jax.shard_map(
        functools.partial(local, groups),
        mesh=mesh,
        in_specs=(P("band", "grid", None), P()),
        out_specs=P("band", "grid", None),
        check_vma=False,
    )
```

```python
import functools
import math

import jax
import jax.numpy as jnp
import numpy as np
from jax import lax
from jax.experimental import pallas as pl
from jax.experimental.pallas import tpu as pltpu
from jax.sharding import PartitionSpec as P

MESH = pl.DeviceIdType.MESH
MIXING = 0.25
BOX_LENGTH = 16.0
SKEW = 4

HALVES = 2
SMALL = ((0, 0, 1), (0, 1, 1), (0, 2, 2), (0, 4, 4), (1, 0, 8))
HALF = ((0, 0, 8), (1, 0, 8))


TAIL = ((0, 0, 8), (1, 0, 4), (1, 4, 2), (1, 6, 2))


def pieces(cuts):
    return [(k, row, 1, column, parts) for k, cut in enumerate(cuts) for row, column, parts in cut]


AHEAD = BACK = pieces((SMALL, HALF, HALF, TAIL))
JOINED_BEFORE = (0, (2, 0, 1, 0, 8))


def in_order_of_arrival(cuts):
    hop, delay, sent, free, events = 0.3, 1.0, 0.0, 0.0, []
    for m, piece in enumerate(cuts):
        size = piece[4] / 16
        sent += size
        free = max(free, sent + hop) + size
        events += [(sent + hop, 0, m), (free + hop + delay, 1, m)]
    return [(what, m) for _, what, m in sorted(events)]

PEER = 0
CROSS = PEER + 3
RELAY = CROSS + 3 * HALVES
DOWN = RELAY + 3 * HALVES
SIDE = DOWN + len(AHEAD)
SIDE_BACK = SIDE + len(AHEAD)
UP_BACK = SIDE_BACK + len(BACK)
JOINT = UP_BACK + len(BACK)
COMB = JOINT + 3
FROM_PEER = COMB + 2
FROM_CHIP = FROM_PEER + 3
FAR = FROM_CHIP + 3
COPIES = FAR + 1


def transform_tables(n):
    ids = np.arange(n)
    angles = (ids[:, None] * ids[None, :] % n) * (2.0 * np.pi / n)
    cas = np.cos(angles) + np.sin(angles)
    high = cas.astype(jnp.bfloat16).astype(np.float64)
    low = cas - high
    none = np.zeros_like(high)
    left = np.block([[high, high], [low, none]])
    both = lambda m: np.block([[m, none], [none, m]])
    right = np.block([[both(high), both(low)], [both(high), np.zeros((2 * n, 2 * n))]])
    return jnp.asarray(left, jnp.bfloat16), jnp.asarray(right, jnp.bfloat16)


def split(values, axis):
    high = values.astype(jnp.bfloat16)
    low = (values - high.astype(jnp.float32)).astype(jnp.bfloat16)
    return jnp.concatenate([high, low], axis=axis)


def left_product(left, values):
    both = jnp.dot(left, split(values, 0), preferred_element_type=jnp.float32)
    half = both.shape[0] // 2
    return both[:half] + both[half:]


def right_product(values, right):
    both = jnp.dot(split(values, 1), right, preferred_element_type=jnp.float32)
    half = both.shape[1] // 2
    return both[:, :half] + both[:, half:]


def fill_coulomb(n, coulomb):
    lanes = 2 * n
    scale = -MIXING * BOX_LENGTH * BOX_LENGTH / math.pi / float(n**3)
    group = 4

    def signed(index):
        return jnp.where(index < n // 2, index, index - n)

    def body(step, carry):
        fy = signed(lax.broadcasted_iota(jnp.int32, (n, lanes), 0))
        fz = signed(lax.broadcasted_iota(jnp.int32, (n, lanes), 1) % n)
        plane = fy * fy + fz * fz
        for u in range(group):
            kx = step * group + u
            fx = signed(kx)
            squared = fx * fx + plane
            safe = jnp.maximum(squared, 1).astype(jnp.float32)
            coulomb[pl.ds(pl.multiple_of(kx * n, n), n), :] = jnp.where(squared > 0, scale / safe, 0.0)
        return carry

    lax.fori_loop(0, n // group, body, 0)


def densities(n, planes, phi, work, right_ref, quarter, pairs):
    lanes, half, stride = 2 * n, n // 2, n + SKEW
    (ia, ta, wa), (ib, tb, wb) = pairs
    start = quarter * planes
    rows = pl.ds(pl.multiple_of(start, planes), planes)
    lower = lax.broadcasted_iota(jnp.int32, (planes, lanes), 1) < n
    right = right_ref[...]
    block = half // 2
    for first_col in range(0, half, block):
        strips = []
        for c in range(first_col, first_col + block):
            cols = slice(c * lanes, (c + 1) * lanes)
            first = phi[ia, rows, cols] * phi[ta, rows, cols] * wa
            second = phi[ib, rows, cols] * phi[tb, rows, cols] * wb
            turned = pltpu.roll(jnp.where(lower, second, first), n, 1)
            strips += [jnp.where(lower, first, turned), jnp.where(lower, turned, second)]
        along_z = right_product(jnp.concatenate(strips, axis=0), right)
        for u in range(2 * block):
            y = 2 * first_col + u
            work[pl.ds(y * stride + start, planes), :] = along_z[u * planes:(u + 1) * planes]


def along_y(n, planes, works, left_ref, quarter):
    stride = n + SKEW
    left = left_ref[...]
    for work in works:
        for u in range(planes // 2):
            here = [pl.ds(quarter * planes + 2 * u + j, n, stride=stride) for j in range(2)]
            done = left_product(left, jnp.concatenate([work[h, :] for h in here], axis=1))
            work[here[0], :] = done[:, :2 * n]
            work[here[1], :] = done[:, 2 * n:]


def along_x(n, work, coulomb, left_ref):
    stride = n + SKEW
    left = left_ref[...]
    for u in range(n // 2):
        here = [pl.ds((2 * u + j) * stride, n) for j in range(2)]
        factor = [coulomb[(2 * u + j) * n:(2 * u + j + 1) * n, :] for j in range(2)]
        spectrum = left_product(left, jnp.concatenate([work[h, :] for h in here], axis=1))
        done = left_product(left, spectrum * jnp.concatenate(factor, axis=1))
        work[here[0], :] = done[:, :2 * n]
        work[here[1], :] = done[:, 2 * n:]


def exchange_terms(n, planes, phi, pot, work, right_ref, quarter, last, partners):
    lanes, half, stride = 2 * n, n // 2, n + SKEW
    start = quarter * planes
    rows = pl.ds(pl.multiple_of(start, planes), planes)
    lower = lax.broadcasted_iota(jnp.int32, (planes, lanes), 1) < n
    right = right_ref[...]
    within = last.astype(jnp.float32)
    block = half // 4
    for first_col in range(0, half, block):
        solved = []
        for p in range(3):
            strips = [work[p, pl.ds(y * stride + start, planes), :]
                      for y in range(2 * first_col, 2 * (first_col + block))]
            solved.append(right_product(jnp.concatenate(strips, axis=0), right))
        for u in range(block):
            cols = slice((first_col + u) * lanes, (first_col + u + 1) * lanes)
            values = []
            for along_z in solved:
                even = along_z[2 * u * planes:(2 * u + 1) * planes]
                odd = along_z[(2 * u + 1) * planes:(2 * u + 2) * planes]
                turned = pltpu.roll(jnp.where(lower, odd, even), n, 1)
                values += [jnp.where(lower, even, turned), jnp.where(lower, turned, odd)]
            away, near = values[:3], values[3:]
            own = [phi[i, rows, cols] for i in range(3)]
            for i in range(3):
                before = (i + 2) % 3
                pot[i, rows, cols] = (away[i] * phi[partners[0][i], rows, cols]
                                      + near[i] * phi[partners[1][i], rows, cols]
                                      + away[before] * own[before] * within)
            pot[3, rows, cols] = near[0] * own[0] + near[1] * own[1] + near[2] * own[2]
            pot[4, rows, cols] = away[0] * own[0] + away[1] * own[1] + away[2] * own[2]


def kernel(groups, mask_hbm, mine_ref, left_hbm, right_hbm, out_ref,
           phi, pot, coulomb, work, side, up, comb, joint, from_peer, from_chip, result,
           left_ref, right_ref, mask_ref, load_sem, send_sem, recv_sem):
    orbs, planes, cells = mine_ref.shape
    n = phi.shape[1]
    band, grid = lax.axis_index("band"), lax.axis_index("grid")
    last = grid // orbs
    odd_band = lax.rem(band, 2)
    below, above = lax.rem(band + groups - 2, groups), lax.rem(band + 2, groups)
    beside = band + 1 - 2 * odd_band
    peer, across, far = grid + 1 - 2 * lax.rem(grid, 2), lax.rem(grid + 2, 4), 3 - grid
    shares, peer_shares = grid < orbs, peer < orbs
    even_shares = shares & (odd_band == 0)
    odd_shares = shares & (odd_band == 1)

    def order(device):
        first, second = 2 * (device // 2), 1 - device // 2
        return first, second, orbs - first - second

    def rows(quarter):
        return pl.ds(pl.multiple_of(quarter * planes, planes), planes)

    depth, width = planes // 2, cells // 8

    def inner(piece):
        _, row, halves, column, parts = piece
        return pl.ds(row * depth, halves * depth), pl.ds(column * width, parts * width)

    def part(quarter, piece):
        _, row, halves, column, parts = piece
        first = pl.multiple_of(quarter * planes + row * depth, depth)
        return pl.ds(first, halves * depth), pl.ds(column * width, parts * width)

    def half(quarter, c):
        return pl.ds(pl.multiple_of(quarter * planes + c * depth, depth), depth)

    def copy(source, target, number, device, sent=None):
        return pltpu.make_async_remote_copy(
            src_ref=source, dst_ref=target, send_sem=send_sem.at[number if sent is None else sent],
            recv_sem=recv_sem.at[number], device_id=device, device_id_type=MESH)

    def arrived(target, number):
        copy(target, target, number, (band, peer)).wait_recv()

    def gone(target, number):
        copy(target, target, number, (band, peer)).wait_send()

    loads = [pltpu.make_async_copy(mine_ref.at[i], phi.at[i, rows(grid)], load_sem.at[i]) for i in range(orbs)]
    loads += [pltpu.make_async_copy(a, b, load_sem.at[orbs + k]) for k, (a, b) in enumerate(
        ((mask_hbm, mask_ref), (left_hbm, left_ref), (right_hbm, right_ref)))]
    for load in loads:
        load.start()

    barrier = pltpu.get_barrier_semaphore()
    for device in ((band, peer), (band, across), (band, far), (beside, grid), (below, grid), (above, grid)):
        pl.semaphore_signal(barrier, inc=1, device_id=device, device_id_type=MESH)
    for load in loads[:orbs]:
        load.wait()
    pl.semaphore_wait(barrier, 6)

    quarters = (grid, peer, across, far)

    def pass_on(k, only=None):
        for m, piece in enumerate(AHEAD):
            if piece[0] != k or only not in (None, piece[1]):
                continue
            here = part(quarters[k], piece)
            source = phi.at[lax.rem(grid, orbs), *here]

            @pl.when(shares)
            def _():
                copy(source, phi.at[4, *here], DOWN + m, (below, grid)).start()

            @pl.when(odd_shares)
            def _():
                copy(source, phi.at[3, *here], SIDE + m, (beside, grid)).start()

    def side_relay(m):
        here = part(quarters[AHEAD[m][0]], AHEAD[m])

        @pl.when(even_shares)
        def _():
            arrived(phi.at[4, *here], DOWN + m)
            copy(phi.at[4, *here], phi.at[3, *here], SIDE + m, (beside, grid)).start()

    def side_relays(k):
        return [m for m, piece in enumerate(AHEAD) if piece[0] == k]

    first_turn, second_turn = grid != 1, grid == 1
    pl.when(first_turn)(lambda: pass_on(0))
    for k, i in enumerate(order(across)):
        for c in range(HALVES):
            piece = phi.at[i, half(grid, c)]
            copy(piece, piece, CROSS + k * HALVES + c, (band, across)).start()
    for k, i in enumerate(order(peer)):
        piece = phi.at[i, rows(grid)]
        copy(piece, piece, PEER + k, (band, peer)).start()

    mine, theirs = order(grid), order(peer)
    for k in range(orbs):
        arrived(phi.at[mine[k], rows(peer)], PEER + k)
    pl.when(first_turn)(lambda: pass_on(1))
    fill_coulomb(n, coulomb)
    for load in loads[orbs:]:
        load.wait()

    def relay(k, c):
        piece = phi.at[mine[k], half(across, c)]
        arrived(piece, CROSS + k * HALVES + c)
        copy(piece, piece, RELAY + k * HALVES + c, (band, peer)).start()

    wanted = lax.rem(grid, 2)

    def far_on(c):
        @pl.when(shares)
        def _():
            arrived(phi.at[grid, half(far, c)], RELAY + wanted * HALVES + c)

        pass_on(3, c)

    def partner(i, near):
        within = lax.rem(i + 1 - near, orbs)
        return last * within + (1 - last) * (4 - near)

    def density(p, quarter):
        pairs = []
        for lane_half in range(2):
            number = 2 * p + lane_half
            near, i = number // orbs, lax.rem(number, orbs)
            ahead = lax.rem(band + 2 - near, groups)
            column = last * (band * orbs + lax.rem(i + 1 - near, orbs)) + (1 - last) * (ahead * orbs + grid)
            weight = mask_ref[band * orbs + i, column].astype(jnp.float32)
            pairs.append((i, partner(i, near), weight))
        densities(n, planes, phi, work.at[p], right_ref, quarter, pairs)

    def await_down(k):
        @pl.when(odd_shares)
        def _():
            for m in side_relays(k):
                arrived(phi.at[4, *part(quarters[k], AHEAD[m])], DOWN + m)

    def await_side(k):
        @pl.when(shares)
        def _():
            for m in side_relays(k):
                arrived(phi.at[3, *part(quarters[k], AHEAD[m])], SIDE + m)

    def choose(index, values):
        chosen = values[0]
        for position, value in enumerate(values[1:], 1):
            chosen = jnp.where(index == position, value, chosen)
        return chosen

    def relayed(k, rows_only=None):
        for m in side_relays(k):
            if rows_only in (None, AHEAD[m][1]):
                side_relay(m)

    def all_relayed():
        for k in range(orbs):
            @pl.when((last == 1) | (k != wanted))
            def _():
                for c in range(HALVES):
                    arrived(phi.at[theirs[k], half(far, c)], RELAY + k * HALVES + c)

    def early_0():
        relayed(0, 0)
        relay(0, 0)
        pass_on(2, 0)
        relayed(0, 1)
        far_on(0)
        await_down(0)

    def early_1():
        relayed(1, 0)
        relay(0, 1)
        pass_on(2, 1)
        relayed(1, 1)
        far_on(1)
        await_down(1)

    def early_2():
        relayed(2, 0)
        await_side(0)

    def early_3():
        relayed(2, 1)
        relay(1, 0)
        await_side(1)

    def early_4():
        relayed(3)
        relay(1, 1)
        relay(2, 0)
        relay(2, 1)
        await_down(2)

    def early_6():
        all_relayed()
        await_down(3)

    def late_0():
        for k in range(2):
            for c in range(HALVES):
                relay(k, c)
        for k in range(3):
            pass_on(k)
        relayed(0, 0)
        relay(2, 0)
        far_on(0)
        far_on(1)
        relayed(0, 1)
        relay(2, 1)
        await_down(0)

    def late_1():
        relayed(1)
        await_down(1)

    def late_3():
        relayed(2)
        await_side(1)

    def late_5():
        relayed(3, 0)
        await_side(2)

    def late_6():
        relayed(3, 1)
        all_relayed()
        await_down(3)

    first_work, other_works, along = range(3)
    steps = ((first_work, 0), (first_work, 1), (other_works, 0), (other_works, 1), (first_work, 2),
             (other_works, 2), (first_work, 3), (along, 0), (other_works, 3), (along, 1), (along, 2))
    early = {0: early_0, 1: early_1, 2: early_2, 3: early_3, 4: early_4, 5: lambda: await_side(2), 6: early_6}
    late = {0: late_0, 1: late_1, 2: lambda: await_side(0), 3: late_3, 4: lambda: await_down(2),
            5: late_5, 6: late_6}

    def step(index, carry):
        for turn, actions in ((first_turn, early), (second_turn, late)):
            for position, action in actions.items():
                pl.when(turn & (index == position))(action)
        pl.when(index == 8)(lambda: await_side(3))
        kind = choose(index, [which for which, _ in steps])
        number = choose(index, [k for _, k in steps])
        quarter = choose(number, quarters)

        @pl.when(kind == first_work)
        def _():
            density(0, quarter)
            along_y(n, planes, [work.at[0]], left_ref, quarter)

        @pl.when(kind == other_works)
        def _():
            density(1, quarter)
            density(2, quarter)
            along_y(n, planes, [work.at[1], work.at[2]], left_ref, quarter)

        @pl.when(kind == along)
        def _():
            along_x(n, work.at[number], coulomb, left_ref)

        return carry

    lax.fori_loop(0, len(steps), step, 0)

    back = (across, far, peer, grid)
    partners = [[partner(i, near) for i in range(3)] for near in range(2)]

    def up_send(m):
        here = part(back[BACK[m][0]], BACK[m])
        copy(pot.at[4, *here], up.at[*here], UP_BACK + m, (above, grid)).start()

    def elsewhere(i):
        return grid // 2 != i // 2

    def send_back(k):
        @pl.when(shares)
        def _():
            for m, piece in enumerate(BACK):
                if piece[0] == k:
                    here = part(back[k], piece)
                    copy(pot.at[3, *here], side.at[*here], SIDE_BACK + m, (beside, grid)).start()

        @pl.when(odd_shares)
        def _():
            for m, piece in enumerate(BACK):
                if piece[0] == k:
                    up_send(m)

        if k == 1:
            for i in range(orbs):
                @pl.when(elsewhere(i))
                def _():
                    copy(pot.at[i, rows(far)], joint.at[i], JOINT + i, (band, peer)).start()

        if k < 2:
            @pl.when(peer_shares)
            def _():
                copy(pot.at[peer, rows(back[k])], comb.at[1 - k], COMB + 1 - k, (band, peer)).start()

        if k == 2:
            for i in range(orbs):
                @pl.when(elsewhere(i) | (peer == i))
                def _():
                    copy(pot.at[i, rows(peer)], from_peer.at[i], FROM_PEER + i, (band, peer)).start()

    def back_step(index, carry):
        quarter = choose(index, back)

        along_y(n, planes, [work.at[p] for p in range(3)], left_ref, quarter)
        exchange_terms(n, planes, phi, pot, work, right_ref, quarter, last, partners)
        for k in range(4):
            pl.when(index == k)(functools.partial(send_back, k))
        return carry

    lax.fori_loop(0, 4, back_step, 0)

    def join(m):
        here = part(back[BACK[m][0]], BACK[m])

        @pl.when(even_shares)
        def _():
            arrived(side.at[*here], SIDE_BACK + m)
            pot[4, *here] += side[*here]
            up_send(m)

    def collect(m):
        k = BACK[m][0]
        here, within = part(back[k], BACK[m]), inner(BACK[m])

        @pl.when(shares)
        def _():
            if k < 2 and BACK[m - 1][0] != k:
                arrived(comb.at[k], COMB + k)
            arrived(up.at[*here], UP_BACK + m)
            if k < 2:
                pot[grid, *here] += up[*here] + comb[k, *within]
            else:
                pot[grid, *here] += up[*here]

        @pl.when(odd_shares)
        def _():
            arrived(side.at[*here], SIDE_BACK + m)
            pot[grid, *here] += side[*here]

        @pl.when(shares)
        def _():
            source = pot.at[grid, *here]
            if k == 0:
                copy(source, from_chip.at[grid, *within], FROM_CHIP + grid, (band, across)).start()
            elif k == 1:
                copy(source, from_chip.at[grid, *within], FROM_CHIP + grid, (band, far), FAR).start()
            elif k == 2:
                copy(source, from_peer.at[grid, *within], FROM_PEER + grid, (band, peer)).start()

    def finish(i, k):
        arrived(from_peer.at[i], FROM_PEER + i)
        arrived(from_chip.at[i], FROM_CHIP + i)
        result[i] = pot[i, rows(grid), :] + from_peer[i] + from_chip[i]
        pltpu.make_async_copy(result.at[i], out_ref.at[i], load_sem.at[k]).start()

    def joined():
        for i in range(orbs):
            @pl.when(elsewhere(i))
            def _():
                arrived(joint.at[i], JOINT + i)
                pot[i, rows(across), :] += joint[i]
                copy(pot.at[i, rows(across)], from_chip.at[i], FROM_CHIP + i, (band, across)).start()

    for what, m in in_order_of_arrival(BACK):
        if (what, BACK[m]) == JOINED_BEFORE:
            joined()
        (collect if what else join)(m)
    soon = choose(grid, (2, 2, 0, 0))
    own = choose(grid, (0, 1, 2, 2))
    for k, i in enumerate((soon, orbs - soon - own, own)):
        finish(i, k)

    whole, halved = comb.at[0], comb.at[0, pl.ds(0, planes // HALVES)]
    for number in range(PEER, PEER + 3):
        gone(whole, number)
    for number in range(CROSS, DOWN):
        gone(halved, number)

    @pl.when(shares)
    def _():
        for first, cuts in ((DOWN, AHEAD), (SIDE, AHEAD), (SIDE_BACK, BACK), (UP_BACK, BACK)):
            for m, piece in enumerate(cuts):
                gone(comb.at[0, *inner(piece)], first + m)
        for number in (FROM_CHIP + grid, FROM_PEER + grid, FAR):
            gone(whole, number)

    @pl.when(peer_shares)
    def _():
        for number in (COMB, COMB + 1, FROM_PEER + peer):
            gone(whole, number)

    for i in range(orbs):
        @pl.when(elsewhere(i))
        def _():
            for number in (JOINT + i, FROM_PEER + i, FROM_CHIP + i):
                gone(whole, number)

    for k in range(orbs):
        pltpu.make_async_copy(result.at[k], out_ref.at[k], load_sem.at[k]).wait()


def local(groups, orbitals, pair_mask):
    orbs, planes, cells = orbitals.shape
    n = math.isqrt(cells)
    left, right = transform_tables(n)
    in_hbm = pl.BlockSpec(memory_space=pltpu.HBM)
    cube, piece = (n, cells), (planes, cells)
    return pl.pallas_call(
        functools.partial(kernel, groups),
        out_shape=jax.ShapeDtypeStruct(orbitals.shape, jnp.float32),
        in_specs=[in_hbm] * 4,
        out_specs=in_hbm,
        scratch_shapes=[
            pltpu.VMEM((orbs + 2, *cube), jnp.float32),
            pltpu.VMEM((orbs + 2, *cube), jnp.float32),
            pltpu.VMEM((n * n, 2 * n), jnp.float32),
            pltpu.VMEM((3, n * (n + SKEW), 2 * n), jnp.float32),
            pltpu.VMEM(cube, jnp.float32),
            pltpu.VMEM(cube, jnp.float32),
            pltpu.VMEM((2, *piece), jnp.float32),
            pltpu.VMEM((orbs, *piece), jnp.float32),
            pltpu.VMEM((orbs, *piece), jnp.float32),
            pltpu.VMEM((orbs, *piece), jnp.float32),
            pltpu.VMEM((orbs, *piece), jnp.float32),
            pltpu.VMEM(left.shape, jnp.bfloat16),
            pltpu.VMEM(right.shape, jnp.bfloat16),
            pltpu.SMEM(pair_mask.shape, jnp.int32),
            pltpu.SemaphoreType.DMA((orbs + 3,)),
            pltpu.SemaphoreType.DMA((COPIES,)),
            pltpu.SemaphoreType.DMA((COPIES,)),
        ],
        compiler_params=pltpu.CompilerParams(
            collective_id=0, has_side_effects=True),
    )(pair_mask, orbitals, left, right)


def solution(mesh):
    groups, parts = mesh.shape["band"], mesh.shape["grid"]
    assert parts == 4 and groups % 2 == 0 and groups >= 4
    return jax.shard_map(
        functools.partial(local, groups),
        mesh=mesh,
        in_specs=(P("band", "grid", None), P()),
        out_specs=P("band", "grid", None),
        check_vma=False,
    )
```

```python
import functools
import math

import jax
import jax.numpy as jnp
import numpy as np
from jax import lax
from jax.experimental import pallas as pl
from jax.experimental.pallas import tpu as pltpu
from jax.sharding import PartitionSpec as P

MESH = pl.DeviceIdType.MESH
MIXING = 0.25
BOX_LENGTH = 16.0
SKEW = 4

HALVES = 2
HALF = ((0, 0, 8), (1, 0, 8))


def pieces(cuts):
    return [(k, row, 1, column, parts) for k, cut in enumerate(cuts) for row, column, parts in cut]


AHEAD = BACK = pieces((HALF, HALF, HALF, HALF))
JOINED_BEFORE = (0, (2, 0, 1, 0, 8))


def in_order_of_arrival(cuts):
    hop, delay, sent, free, events = 0.3, 1.0, 0.0, 0.0, []
    for m, piece in enumerate(cuts):
        size = piece[4] / 16
        sent += size
        free = max(free, sent + hop) + size
        events += [(sent + hop, 0, m), (free + hop + delay, 1, m)]
    return [(what, m) for _, what, m in sorted(events)]

PEER = 0
CROSS = PEER + 3
RELAY = CROSS + 3 * HALVES
DOWN = RELAY + 3 * HALVES
SIDE = DOWN + len(AHEAD)
SIDE_BACK = SIDE + len(AHEAD)
UP_BACK = SIDE_BACK + len(BACK)
JOINT = UP_BACK + len(BACK)
COMB = JOINT + 3
FROM_PEER = COMB + 2
FROM_CHIP = FROM_PEER + 3
FAR = FROM_CHIP + 3
COPIES = FAR + 1


def transform_tables(n):
    ids = np.arange(n)
    angles = (ids[:, None] * ids[None, :] % n) * (2.0 * np.pi / n)
    cas = np.cos(angles) + np.sin(angles)
    high = cas.astype(jnp.bfloat16).astype(np.float64)
    low = cas - high
    none = np.zeros_like(high)
    left = np.block([[high, high], [low, none]])
    both = lambda m: np.block([[m, none], [none, m]])
    right = np.block([[both(high), both(low)], [both(high), np.zeros((2 * n, 2 * n))]])
    return jnp.asarray(left, jnp.bfloat16), jnp.asarray(right, jnp.bfloat16)


def split(values, axis):
    high = values.astype(jnp.bfloat16)
    low = (values - high.astype(jnp.float32)).astype(jnp.bfloat16)
    return jnp.concatenate([high, low], axis=axis)


def left_product(left, values):
    both = jnp.dot(left, split(values, 0), preferred_element_type=jnp.float32)
    half = both.shape[0] // 2
    return both[:half] + both[half:]


def right_product(values, right):
    both = jnp.dot(split(values, 1), right, preferred_element_type=jnp.float32)
    half = both.shape[1] // 2
    return both[:, :half] + both[:, half:]


def fill_coulomb(n, coulomb):
    lanes = 2 * n
    scale = -MIXING * BOX_LENGTH * BOX_LENGTH / math.pi / float(n**3)
    group = 4

    def signed(index):
        return jnp.where(index < n // 2, index, index - n)

    def body(step, carry):
        fy = signed(lax.broadcasted_iota(jnp.int32, (n, lanes), 0))
        fz = signed(lax.broadcasted_iota(jnp.int32, (n, lanes), 1) % n)
        plane = fy * fy + fz * fz
        for u in range(group):
            kx = step * group + u
            fx = signed(kx)
            squared = fx * fx + plane
            safe = jnp.maximum(squared, 1).astype(jnp.float32)
            coulomb[pl.ds(pl.multiple_of(kx * n, n), n), :] = jnp.where(squared > 0, scale / safe, 0.0)
        return carry

    lax.fori_loop(0, n // group, body, 0)


def densities(n, planes, phi, work, right_ref, quarter, pairs):
    lanes, half, stride = 2 * n, n // 2, n + SKEW
    (ia, ta, wa), (ib, tb, wb) = pairs
    start = quarter * planes
    rows = pl.ds(pl.multiple_of(start, planes), planes)
    lower = lax.broadcasted_iota(jnp.int32, (planes, lanes), 1) < n
    right = right_ref[...]
    block = half // 2
    for first_col in range(0, half, block):
        strips = []
        for c in range(first_col, first_col + block):
            cols = slice(c * lanes, (c + 1) * lanes)
            first = phi[ia, rows, cols] * phi[ta, rows, cols] * wa
            second = phi[ib, rows, cols] * phi[tb, rows, cols] * wb
            turned = pltpu.roll(jnp.where(lower, second, first), n, 1)
            strips += [jnp.where(lower, first, turned), jnp.where(lower, turned, second)]
        along_z = right_product(jnp.concatenate(strips, axis=0), right)
        for u in range(2 * block):
            y = 2 * first_col + u
            work[pl.ds(y * stride + start, planes), :] = along_z[u * planes:(u + 1) * planes]


def along_y(n, planes, works, left_ref, quarter):
    stride = n + SKEW
    left = left_ref[...]
    for work in works:
        for u in range(planes // 2):
            here = [pl.ds(quarter * planes + 2 * u + j, n, stride=stride) for j in range(2)]
            done = left_product(left, jnp.concatenate([work[h, :] for h in here], axis=1))
            work[here[0], :] = done[:, :2 * n]
            work[here[1], :] = done[:, 2 * n:]


def along_x(n, work, coulomb, left_ref):
    stride = n + SKEW
    left = left_ref[...]
    for u in range(n // 2):
        here = [pl.ds((2 * u + j) * stride, n) for j in range(2)]
        factor = [coulomb[(2 * u + j) * n:(2 * u + j + 1) * n, :] for j in range(2)]
        spectrum = left_product(left, jnp.concatenate([work[h, :] for h in here], axis=1))
        done = left_product(left, spectrum * jnp.concatenate(factor, axis=1))
        work[here[0], :] = done[:, :2 * n]
        work[here[1], :] = done[:, 2 * n:]


def exchange_terms(n, planes, phi, pot, work, right_ref, quarter, last, partners):
    lanes, half, stride = 2 * n, n // 2, n + SKEW
    start = quarter * planes
    rows = pl.ds(pl.multiple_of(start, planes), planes)
    lower = lax.broadcasted_iota(jnp.int32, (planes, lanes), 1) < n
    right = right_ref[...]
    within = last.astype(jnp.float32)
    block = half // 4
    for first_col in range(0, half, block):
        solved = []
        for p in range(3):
            strips = [work[p, pl.ds(y * stride + start, planes), :]
                      for y in range(2 * first_col, 2 * (first_col + block))]
            solved.append(right_product(jnp.concatenate(strips, axis=0), right))
        for u in range(block):
            cols = slice((first_col + u) * lanes, (first_col + u + 1) * lanes)
            values = []
            for along_z in solved:
                even = along_z[2 * u * planes:(2 * u + 1) * planes]
                odd = along_z[(2 * u + 1) * planes:(2 * u + 2) * planes]
                turned = pltpu.roll(jnp.where(lower, odd, even), n, 1)
                values += [jnp.where(lower, even, turned), jnp.where(lower, turned, odd)]
            away, near = values[:3], values[3:]
            own = [phi[i, rows, cols] for i in range(3)]
            for i in range(3):
                before = (i + 2) % 3
                pot[i, rows, cols] = (away[i] * phi[partners[0][i], rows, cols]
                                      + near[i] * phi[partners[1][i], rows, cols]
                                      + away[before] * own[before] * within)
            pot[3, rows, cols] = near[0] * own[0] + near[1] * own[1] + near[2] * own[2]
            pot[4, rows, cols] = away[0] * own[0] + away[1] * own[1] + away[2] * own[2]


def kernel(groups, mask_hbm, mine_ref, left_hbm, right_hbm, out_ref,
           phi, pot, coulomb, work, side, up, comb, joint, from_peer, from_chip, result,
           left_ref, right_ref, mask_ref, load_sem, send_sem, recv_sem):
    orbs, planes, cells = mine_ref.shape
    n = phi.shape[1]
    band, grid = lax.axis_index("band"), lax.axis_index("grid")
    last = grid // orbs
    odd_band = lax.rem(band, 2)
    below, above = lax.rem(band + groups - 2, groups), lax.rem(band + 2, groups)
    beside = band + 1 - 2 * odd_band
    peer, across, far = grid + 1 - 2 * lax.rem(grid, 2), lax.rem(grid + 2, 4), 3 - grid
    shares, peer_shares = grid < orbs, peer < orbs
    even_shares = shares & (odd_band == 0)
    odd_shares = shares & (odd_band == 1)

    def order(device):
        first, second = 2 * (device // 2), 1 - device // 2
        return first, second, orbs - first - second

    def rows(quarter):
        return pl.ds(pl.multiple_of(quarter * planes, planes), planes)

    depth, width = planes // 2, cells // 8

    def inner(piece):
        _, row, halves, column, parts = piece
        return pl.ds(row * depth, halves * depth), pl.ds(column * width, parts * width)

    def part(quarter, piece):
        _, row, halves, column, parts = piece
        first = pl.multiple_of(quarter * planes + row * depth, depth)
        return pl.ds(first, halves * depth), pl.ds(column * width, parts * width)

    def half(quarter, c):
        return pl.ds(pl.multiple_of(quarter * planes + c * depth, depth), depth)

    def copy(source, target, number, device, sent=None):
        return pltpu.make_async_remote_copy(
            src_ref=source, dst_ref=target, send_sem=send_sem.at[number if sent is None else sent],
            recv_sem=recv_sem.at[number], device_id=device, device_id_type=MESH)

    def arrived(target, number):
        copy(target, target, number, (band, peer)).wait_recv()

    def gone(target, number):
        copy(target, target, number, (band, peer)).wait_send()

    loads = [pltpu.make_async_copy(mine_ref.at[i], phi.at[i, rows(grid)], load_sem.at[i]) for i in range(orbs)]
    loads += [pltpu.make_async_copy(a, b, load_sem.at[orbs + k]) for k, (a, b) in enumerate(
        ((mask_hbm, mask_ref), (left_hbm, left_ref), (right_hbm, right_ref)))]
    for load in loads:
        load.start()

    barrier = pltpu.get_barrier_semaphore()
    for device in ((band, peer), (band, across), (band, far), (beside, grid), (below, grid), (above, grid)):
        pl.semaphore_signal(barrier, inc=1, device_id=device, device_id_type=MESH)
    for load in loads[:orbs]:
        load.wait()
    pl.semaphore_wait(barrier, 6)

    quarters = (grid, peer, across, far)

    def pass_on(k, only=None):
        for m, piece in enumerate(AHEAD):
            if piece[0] != k or only not in (None, piece[1]):
                continue
            here = part(quarters[k], piece)
            source = phi.at[lax.rem(grid, orbs), *here]

            @pl.when(shares)
            def _():
                copy(source, phi.at[4, *here], DOWN + m, (below, grid)).start()

            @pl.when(odd_shares)
            def _():
                copy(source, phi.at[3, *here], SIDE + m, (beside, grid)).start()

    def side_relay(m):
        here = part(quarters[AHEAD[m][0]], AHEAD[m])

        @pl.when(even_shares)
        def _():
            arrived(phi.at[4, *here], DOWN + m)
            copy(phi.at[4, *here], phi.at[3, *here], SIDE + m, (beside, grid)).start()

    def side_relays(k):
        return [m for m, piece in enumerate(AHEAD) if piece[0] == k]

    first_turn, second_turn = grid != 1, grid == 1
    pl.when(first_turn)(lambda: pass_on(0))
    for k, i in enumerate(order(across)):
        for c in range(HALVES):
            piece = phi.at[i, half(grid, c)]
            copy(piece, piece, CROSS + k * HALVES + c, (band, across)).start()
    for k, i in enumerate(order(peer)):
        piece = phi.at[i, rows(grid)]
        copy(piece, piece, PEER + k, (band, peer)).start()

    mine, theirs = order(grid), order(peer)
    for k in range(orbs):
        arrived(phi.at[mine[k], rows(peer)], PEER + k)
    pl.when(first_turn)(lambda: pass_on(1))
    fill_coulomb(n, coulomb)
    for load in loads[orbs:]:
        load.wait()

    def relay(k, c):
        piece = phi.at[mine[k], half(across, c)]
        arrived(piece, CROSS + k * HALVES + c)
        copy(piece, piece, RELAY + k * HALVES + c, (band, peer)).start()

    wanted = lax.rem(grid, 2)

    def far_on(c):
        @pl.when(shares)
        def _():
            arrived(phi.at[grid, half(far, c)], RELAY + wanted * HALVES + c)

        pass_on(3, c)

    def partner(i, near):
        within = lax.rem(i + 1 - near, orbs)
        return last * within + (1 - last) * (4 - near)

    def density(p, quarter):
        pairs = []
        for lane_half in range(2):
            number = 2 * p + lane_half
            near, i = number // orbs, lax.rem(number, orbs)
            ahead = lax.rem(band + 2 - near, groups)
            column = last * (band * orbs + lax.rem(i + 1 - near, orbs)) + (1 - last) * (ahead * orbs + grid)
            weight = mask_ref[band * orbs + i, column].astype(jnp.float32)
            pairs.append((i, partner(i, near), weight))
        densities(n, planes, phi, work.at[p], right_ref, quarter, pairs)

    def await_down(k):
        @pl.when(odd_shares)
        def _():
            for m in side_relays(k):
                arrived(phi.at[4, *part(quarters[k], AHEAD[m])], DOWN + m)

    def await_side(k):
        @pl.when(shares)
        def _():
            for m in side_relays(k):
                arrived(phi.at[3, *part(quarters[k], AHEAD[m])], SIDE + m)

    def choose(index, values):
        chosen = values[0]
        for position, value in enumerate(values[1:], 1):
            chosen = jnp.where(index == position, value, chosen)
        return chosen

    def relayed(k, rows_only=None):
        for m in side_relays(k):
            if rows_only in (None, AHEAD[m][1]):
                side_relay(m)

    def all_relayed():
        for k in range(orbs):
            @pl.when((last == 1) | (k != wanted))
            def _():
                for c in range(HALVES):
                    arrived(phi.at[theirs[k], half(far, c)], RELAY + k * HALVES + c)

    def early_0():
        relayed(0, 0)
        relay(0, 0)
        pass_on(2, 0)
        relayed(0, 1)
        far_on(0)
        await_down(0)

    def early_1():
        relayed(1, 0)
        relay(0, 1)
        pass_on(2, 1)
        relayed(1, 1)
        far_on(1)
        await_down(1)

    def early_2():
        relayed(2, 0)
        await_side(0)

    def early_3():
        relayed(2, 1)
        relay(1, 0)
        await_side(1)

    def early_4():
        relayed(3)
        relay(1, 1)
        relay(2, 0)
        relay(2, 1)
        await_down(2)

    def early_6():
        all_relayed()
        await_down(3)

    def late_0():
        for k in range(2):
            for c in range(HALVES):
                relay(k, c)
        for k in range(3):
            pass_on(k)
        relayed(0, 0)
        relay(2, 0)
        far_on(0)
        far_on(1)
        relayed(0, 1)
        relay(2, 1)
        await_down(0)

    def late_1():
        relayed(1)
        await_down(1)

    def late_3():
        relayed(2)
        await_side(1)

    def late_5():
        relayed(3, 0)
        await_side(2)

    def late_6():
        relayed(3, 1)
        all_relayed()
        await_down(3)

    first_work, other_works, along = range(3)
    steps = ((first_work, 0), (first_work, 1), (other_works, 0), (other_works, 1), (first_work, 2),
             (other_works, 2), (first_work, 3), (along, 0), (other_works, 3), (along, 1), (along, 2))
    early = {0: early_0, 1: early_1, 2: early_2, 3: early_3, 4: early_4, 5: lambda: await_side(2), 6: early_6}
    late = {0: late_0, 1: late_1, 2: lambda: await_side(0), 3: late_3, 4: lambda: await_down(2),
            5: late_5, 6: late_6}

    def step(index, carry):
        for turn, actions in ((first_turn, early), (second_turn, late)):
            for position, action in actions.items():
                pl.when(turn & (index == position))(action)
        pl.when(index == 8)(lambda: await_side(3))
        kind = choose(index, [which for which, _ in steps])
        number = choose(index, [k for _, k in steps])
        quarter = choose(number, quarters)

        @pl.when(kind == first_work)
        def _():
            density(0, quarter)
            along_y(n, planes, [work.at[0]], left_ref, quarter)

        @pl.when(kind == other_works)
        def _():
            density(1, quarter)
            density(2, quarter)
            along_y(n, planes, [work.at[1], work.at[2]], left_ref, quarter)

        @pl.when(kind == along)
        def _():
            along_x(n, work.at[number], coulomb, left_ref)

        return carry

    lax.fori_loop(0, len(steps), step, 0)

    back = (across, far, peer, grid)
    partners = [[partner(i, near) for i in range(3)] for near in range(2)]

    def up_send(m):
        here = part(back[BACK[m][0]], BACK[m])
        copy(pot.at[4, *here], up.at[*here], UP_BACK + m, (above, grid)).start()

    def elsewhere(i):
        return grid // 2 != i // 2

    def send_back(k):
        @pl.when(shares)
        def _():
            for m, piece in enumerate(BACK):
                if piece[0] == k:
                    here = part(back[k], piece)
                    copy(pot.at[3, *here], side.at[*here], SIDE_BACK + m, (beside, grid)).start()

        @pl.when(odd_shares)
        def _():
            for m, piece in enumerate(BACK):
                if piece[0] == k:
                    up_send(m)

        if k == 1:
            for i in range(orbs):
                @pl.when(elsewhere(i))
                def _():
                    copy(pot.at[i, rows(far)], joint.at[i], JOINT + i, (band, peer)).start()

        if k < 2:
            @pl.when(peer_shares)
            def _():
                copy(pot.at[peer, rows(back[k])], comb.at[1 - k], COMB + 1 - k, (band, peer)).start()

        if k == 2:
            for i in range(orbs):
                @pl.when(elsewhere(i) | (peer == i))
                def _():
                    copy(pot.at[i, rows(peer)], from_peer.at[i], FROM_PEER + i, (band, peer)).start()

    def back_step(index, carry):
        quarter = choose(index, back)

        along_y(n, planes, [work.at[p] for p in range(3)], left_ref, quarter)
        exchange_terms(n, planes, phi, pot, work, right_ref, quarter, last, partners)
        for k in range(4):
            pl.when(index == k)(functools.partial(send_back, k))
        return carry

    lax.fori_loop(0, 4, back_step, 0)

    def join(m):
        here = part(back[BACK[m][0]], BACK[m])

        @pl.when(even_shares)
        def _():
            arrived(side.at[*here], SIDE_BACK + m)
            pot[4, *here] += side[*here]
            up_send(m)

    def collect(m):
        k = BACK[m][0]
        here, within = part(back[k], BACK[m]), inner(BACK[m])

        @pl.when(shares)
        def _():
            if k < 2 and BACK[m - 1][0] != k:
                arrived(comb.at[k], COMB + k)
            arrived(up.at[*here], UP_BACK + m)
            if k < 2:
                pot[grid, *here] += up[*here] + comb[k, *within]
            else:
                pot[grid, *here] += up[*here]

        @pl.when(odd_shares)
        def _():
            arrived(side.at[*here], SIDE_BACK + m)
            pot[grid, *here] += side[*here]

        @pl.when(shares)
        def _():
            source = pot.at[grid, *here]
            if k == 0:
                copy(source, from_chip.at[grid, *within], FROM_CHIP + grid, (band, across)).start()
            elif k == 1:
                copy(source, from_chip.at[grid, *within], FROM_CHIP + grid, (band, far), FAR).start()
            elif k == 2:
                copy(source, from_peer.at[grid, *within], FROM_PEER + grid, (band, peer)).start()

    def finish(i, k):
        arrived(from_peer.at[i], FROM_PEER + i)
        arrived(from_chip.at[i], FROM_CHIP + i)
        result[i] = pot[i, rows(grid), :] + from_peer[i] + from_chip[i]
        pltpu.make_async_copy(result.at[i], out_ref.at[i], load_sem.at[k]).start()

    def joined():
        for i in range(orbs):
            @pl.when(elsewhere(i))
            def _():
                arrived(joint.at[i], JOINT + i)
                pot[i, rows(across), :] += joint[i]
                copy(pot.at[i, rows(across)], from_chip.at[i], FROM_CHIP + i, (band, across)).start()

    for what, m in in_order_of_arrival(BACK):
        if (what, BACK[m]) == JOINED_BEFORE:
            joined()
        (collect if what else join)(m)
    soon = choose(grid, (2, 2, 0, 0))
    own = choose(grid, (0, 1, 2, 2))
    for k, i in enumerate((soon, orbs - soon - own, own)):
        finish(i, k)

    whole, halved = comb.at[0], comb.at[0, pl.ds(0, planes // HALVES)]
    for number in range(PEER, PEER + 3):
        gone(whole, number)
    for number in range(CROSS, DOWN):
        gone(halved, number)

    @pl.when(shares)
    def _():
        for first, cuts in ((DOWN, AHEAD), (SIDE, AHEAD), (SIDE_BACK, BACK), (UP_BACK, BACK)):
            for m, piece in enumerate(cuts):
                gone(comb.at[0, *inner(piece)], first + m)
        for number in (FROM_CHIP + grid, FROM_PEER + grid, FAR):
            gone(whole, number)

    @pl.when(peer_shares)
    def _():
        for number in (COMB, COMB + 1, FROM_PEER + peer):
            gone(whole, number)

    for i in range(orbs):
        @pl.when(elsewhere(i))
        def _():
            for number in (JOINT + i, FROM_PEER + i, FROM_CHIP + i):
                gone(whole, number)

    for k in range(orbs):
        pltpu.make_async_copy(result.at[k], out_ref.at[k], load_sem.at[k]).wait()


def local(groups, orbitals, pair_mask):
    orbs, planes, cells = orbitals.shape
    n = math.isqrt(cells)
    left, right = transform_tables(n)
    in_hbm = pl.BlockSpec(memory_space=pltpu.HBM)
    cube, piece = (n, cells), (planes, cells)
    return pl.pallas_call(
        functools.partial(kernel, groups),
        out_shape=jax.ShapeDtypeStruct(orbitals.shape, jnp.float32),
        in_specs=[in_hbm] * 4,
        out_specs=in_hbm,
        scratch_shapes=[
            pltpu.VMEM((orbs + 2, *cube), jnp.float32),
            pltpu.VMEM((orbs + 2, *cube), jnp.float32),
            pltpu.VMEM((n * n, 2 * n), jnp.float32),
            pltpu.VMEM((3, n * (n + SKEW), 2 * n), jnp.float32),
            pltpu.VMEM(cube, jnp.float32),
            pltpu.VMEM(cube, jnp.float32),
            pltpu.VMEM((2, *piece), jnp.float32),
            pltpu.VMEM((orbs, *piece), jnp.float32),
            pltpu.VMEM((orbs, *piece), jnp.float32),
            pltpu.VMEM((orbs, *piece), jnp.float32),
            pltpu.VMEM((orbs, *piece), jnp.float32),
            pltpu.VMEM(left.shape, jnp.bfloat16),
            pltpu.VMEM(right.shape, jnp.bfloat16),
            pltpu.SMEM(pair_mask.shape, jnp.int32),
            pltpu.SemaphoreType.DMA((orbs + 3,)),
            pltpu.SemaphoreType.DMA((COPIES,)),
            pltpu.SemaphoreType.DMA((COPIES,)),
        ],
        compiler_params=pltpu.CompilerParams(
            collective_id=0, has_side_effects=True),
    )(pair_mask, orbitals, left, right)


def solution(mesh):
    groups, parts = mesh.shape["band"], mesh.shape["grid"]
    assert parts == 4 and groups % 2 == 0 and groups >= 4
    return jax.shard_map(
        functools.partial(local, groups),
        mesh=mesh,
        in_specs=(P("band", "grid", None), P()),
        out_specs=P("band", "grid", None),
        check_vma=False,
    )
```
